32 devices in a mesh: parts: 2 (over y), gz: 4 (over z), gy: 2 (over x), lc: 2 (over core).
Axes of the slice: x: 2, y: 2, z: 4, core: 2. Of those that a mesh axis runs over, the one named last changes fastest.
Arguments:
- density: float32 [64, 128, 256], P(('parts', 'gz'), 'gy'), parts along dimension 0, may hold values from 0.05 to 1
- void_mask: int32 [64, 128, 256], P(('parts', 'gz'), 'gy'), parts along dimension 0, may hold values 0 or 1
- fixed_mask: int32 [64, 128, 256], P(('parts', 'gz'), 'gy'), parts along dimension 0, may hold values 0 or 1
- displacement: float32 [2, 3, 64, 128, 256], P('lc', None, ('parts', 'gz'), 'gy'), parts along dimension 2, may hold values from -4 to 4
- load_ratio: int32 [4], P('parts'), parts along dimension 0, may hold values from 1 to 8
Outputs:
- gradient: float32 [64, 128, 256], P(('parts', 'gz'), 'gy'), parts along dimension 0
The draws below stay inside these ranges and needn't reach their ends.
There are 2 independent parts, one for each index of `parts`. The reference program is written for one: setup_inputs(seed, part) draws one part's arguments, and reference() takes and returns one part's arrays. A program takes and returns all parts, laid end to end along the dimension named above; each array names one. Nothing has to cross between parts.
All inputs are finite; a program needn't handle non-finite values. No bound on the sum of `void_mask` or of `fixed_mask` on one device may be relied on, other than what follows from the above.
Results may differ from the reference program's by a relative error of at most 0.0001.
Values sent between devices are 32-bit elements; how exact they have to be, the bound alone decides.
No kernel may reach another device: no remote copies, remote signals or barrier semaphores. Data moves between devices by JAX's collectives and lax.ppermute only.
A program may use at most 64 MiB of HBM per device.

```python
import math
import jax
import jax.numpy as jnp
import numpy as np
from jax import lax

NZ = 256
NX = 32
NY = 128
LC = 2


def with_ends(values, rng, low, high):
    dims = values.shape
    spot = [jax.random.randint(jax.random.fold_in(rng, axis), (), 0, dims[axis]) for axis in range(len(dims))]
    values = values.at[tuple(spot)].set(low)
    longest = dims.index(max(dims))
    spot[longest] = (spot[longest] + 1) % dims[longest]
    return values.at[tuple(spot)].set(high)


def block_scale(key, extent, cuts, least, top_value):
    factor_of, own = 1.0, jax.random.fold_in(key, 6)
    for axis_at, shards_of in cuts:
        steps = jnp.exp(jax.random.uniform(jax.random.fold_in(own, axis_at), (shards_of,), jnp.float32, least / len(cuts), top_value / len(cuts)))
        factor_of = factor_of * jnp.repeat(steps, extent[axis_at] // shards_of).reshape([-1 if axis == axis_at else 1 for axis in range(len(extent))])
    return factor_of


def scatter_about(own_key, dims, deviation, bound, cuts=(), kind=jnp.bfloat16):
    gain = block_scale(own_key, dims, cuts, -0.22, 0.18) if cuts else 1.0
    entries = jax.random.normal(own_key, dims, jnp.float32) * deviation * gain
    return jnp.minimum(jnp.maximum(entries, -bound), bound).astype(kind)


def setup_inputs(seed: int = 0, part: int = 0) -> dict:
    key_list = jax.random.split(jax.random.key(seed), 6)
    part_keys = jax.random.split(jax.random.fold_in(key_list[5], part), 6)
    return {
        "density": jnp.clip(0.05 + 0.95 * jax.random.uniform(part_keys[0], (NX, NY, NZ), jnp.float32) ** block_scale(part_keys[0], (NX, NY, NZ), ((0, 4), (1, 2)), -0.2, 0.2), 0.05, 1.0),
        "void_mask": with_ends((jax.random.randint(part_keys[1], (NX, NY, NZ), 0, 8) < 1).astype(jnp.int32), jax.random.fold_in(part_keys[1], 1), 0, 1),
        "fixed_mask": with_ends((jax.random.randint(part_keys[2], (NX, NY, NZ), 0, 8) < 1).astype(jnp.int32), jax.random.fold_in(part_keys[2], 1), 0, 1),
        "displacement": scatter_about(part_keys[3], (LC, 3, NX, NY, NZ), 0.3, 4.0, ((0, 2), (2, 4), (3, 2)), jnp.float32),
        "load_ratio": jax.random.randint(part_keys[4], (LC,), 1, 9).astype(jnp.int32),
    }


def element_stiffness():
    poisson = 0.3
    factor = 1.0 / ((1.0 + poisson) * (1.0 - 2.0 * poisson))
    material = np.zeros((6, 6))
    material[:3, :3] = poisson
    for index in range(3):
        material[index, index] = 1.0 - poisson
        material[index + 3, index + 3] = 0.5 - poisson
    material = material * factor
    corners = [(first, second, third) for first in (0, 1) for second in (0, 1) for third in (0, 1)]
    points = [0.5 - 0.5 / math.sqrt(3.0), 0.5 + 0.5 / math.sqrt(3.0)]
    stiffness = np.zeros((24, 24))
    for point_x in points:
        for point_y in points:
            for point_z in points:
                strain = np.zeros((6, 24))
                for corner_index, (first, second, third) in enumerate(corners):
                    along_x = point_x if first else 1.0 - point_x
                    along_y = point_y if second else 1.0 - point_y
                    along_z = point_z if third else 1.0 - point_z
                    sign_x = 1.0 if first else -1.0
                    sign_y = 1.0 if second else -1.0
                    sign_z = 1.0 if third else -1.0
                    deriv_x = sign_x * along_y * along_z
                    deriv_y = along_x * sign_y * along_z
                    deriv_z = along_x * along_y * sign_z
                    column = 3 * corner_index
                    strain[0, column] = deriv_x
                    strain[1, column + 1] = deriv_y
                    strain[2, column + 2] = deriv_z
                    strain[3, column] = deriv_y
                    strain[3, column + 1] = deriv_x
                    strain[4, column + 1] = deriv_z
                    strain[4, column + 2] = deriv_y
                    strain[5, column] = deriv_z
                    strain[5, column + 2] = deriv_x
                stiffness = stiffness + 0.125 * strain.T @ material @ strain
    return stiffness

def cone_offsets():
    result = []
    for shift_x in range(-2, 3):
        for shift_y in range(-2, 3):
            for shift_z in range(-2, 3):
                dist_sq = shift_x * shift_x + shift_y * shift_y + shift_z * shift_z
                if dist_sq < 6.25:
                    result.append((shift_x, shift_y, shift_z, 2.5 - math.sqrt(dist_sq)))
    return result

def cone_filter(padded, shape):
    rows_x, rows_y, depth = shape
    total = jnp.zeros(shape, padded.dtype)
    for shift_x, shift_y, shift_z, weight in cone_offsets():
        total = total + weight * padded[2 + shift_x:2 + shift_x + rows_x, 2 + shift_y:2 + shift_y + rows_y, 2 + shift_z:2 + shift_z + depth]
    return total

def strain_energy(moved):
    rows_x, rows_y, depth = (moved.shape[1], moved.shape[2], moved.shape[3])
    extended = jnp.pad(moved, ((0, 0), (0, 1), (0, 1), (0, 1)))
    stiffness = jnp.asarray(element_stiffness(), moved.dtype)

    def one_layer(layer):
        layers = lax.dynamic_slice_in_dim(extended, layer, 2, 1)
        nodes = []
        for first in (0, 1):
            for second in (0, 1):
                for third in (0, 1):
                    nodes.append(layers[:, first, second:second + rows_y, third:third + depth])
        flat = jnp.stack(nodes, 0).reshape(24, rows_y * depth)
        product = jnp.dot(stiffness, flat, precision=lax.Precision.HIGHEST)
        return lax.optimization_barrier(jnp.sum(flat * product, 0)).reshape(rows_y, depth)
    return lax.map(one_layer, jnp.arange(rows_x, dtype=jnp.int32))

def reference(density, void_mask, fixed_mask, displacement, load_ratio):
    shape = density.shape
    weight_sum = cone_filter(jnp.pad(jnp.ones_like(density), 2), shape)
    physical = cone_filter(jnp.pad(density, 2), shape) / weight_sum
    free = (1 - fixed_mask).astype(density.dtype)
    ratios = load_ratio.astype(density.dtype)
    shares = ratios / jnp.sum(ratios)
    weighted = jnp.zeros(shape, density.dtype)
    for case in range(displacement.shape[0]):
        energy = strain_energy(displacement[case] * free[None])
        weighted = weighted + shares[case] * energy
    alive = (1 - void_mask).astype(density.dtype)
    sensed = alive * (-3.0 * physical * physical * (1.0 - 0.001)) * weighted / weight_sum
    return alive * cone_filter(jnp.pad(sensed, 2), shape)
```

```python
import functools
import math

import jax
import jax.numpy as jnp
import numpy as np
from jax import lax
from jax.experimental import pallas as pl
from jax.experimental.pallas import tpu as pltpu
from jax.sharding import PartitionSpec as P

TILE = 8
SLOT = 4
WEIGHT = [2.5 - math.sqrt(squared) for squared in range(7)]


def energy_factors():
    poisson = 0.3
    factor = 1.0 / ((1.0 + poisson) * (1.0 - 2.0 * poisson))
    shear = factor * (0.5 - poisson) / 16.0
    bulk = factor * poisson / 16.0
    twist = factor * (0.5 - poisson) / 48.0
    warp = factor * ((1.0 - poisson) + 2.0 * (0.5 - poisson)) / 144.0
    return shear, bulk, twist, warp


def filled(shape, value=0.0):
    return jnp.full(shape, value, jnp.float32)


def along_depth(field, offset):
    depth = field.shape[-1]
    position = lax.broadcasted_iota(jnp.int32, field.shape, 1)
    keep = position < depth - offset if offset > 0 else position >= -offset
    return jnp.where(keep, pltpu.roll(field, (-offset) % depth, 1), 0.0)


def combined(y0, y1, y2, at):
    plain = y0[at]
    near = (y0[at - 1] + y0[at + 1]) + y1[at]
    corner = y1[at - 1] + y1[at + 1]
    far = (y0[at - 2] + y0[at + 2]) + y2[at]
    knight = (y2[at - 1] + y2[at + 1]) + (y1[at - 2] + y1[at + 2])
    return plain, near, corner, far, knight


def depth_levels(plain, near, corner, far, knight):
    w = WEIGHT
    level0 = w[0] * plain + w[1] * near + w[2] * corner + w[4] * far + w[5] * knight
    level1 = w[1] * plain + w[2] * near + w[3] * corner + w[5] * far + w[6] * knight
    level2 = w[4] * plain + w[5] * near + w[6] * corner
    return level0, level1, level2


def cone_rows(source, row, count):
    y0, y1, y2 = [], [], []
    for layer in range(count + 4):
        here = source[layer, pl.ds(row, TILE), :]
        one = source[layer, pl.ds(row - 1, TILE), :] + source[layer, pl.ds(row + 1, TILE), :]
        y0.append(here)
        y1.append(one)
        if 1 <= layer <= count + 2:
            y2.append(source[layer, pl.ds(row - 2, TILE), :] + source[layer, pl.ds(row + 2, TILE), :])
        else:
            y2.append(None)
        if layer >= 4:
            level0, level1, level2 = depth_levels(*combined(y0, y1, y2, layer - 2))
            total = level0 + (along_depth(level1, 1) + along_depth(level1, -1))
            yield layer - 4, total + (along_depth(level2, 2) + along_depth(level2, -2))


def node_modes(source, layer, row, components=3):
    modes = []
    for component in range(components):
        low = source[component, layer, pl.ds(row, TILE), :]
        high = source[component, layer, pl.ds(row + 1, TILE), :]
        for value in (low + high, high - low):
            after = along_depth(value, 1)
            modes.append(value + after)
            modes.append(after - value)
    return modes


def element_energy(lower, upper):
    shear, bulk, twist, warp = energy_factors()

    def mode(component, first, second, third):
        index = 4 * component + 2 * second + third
        if first:
            return upper[index] - lower[index]
        return upper[index] + lower[index]

    def square(value):
        return value * value

    normal = [mode(0, 1, 0, 0), mode(1, 0, 1, 0), mode(2, 0, 0, 1)]
    trace = normal[0] + normal[1] + normal[2]
    sheared = [
        mode(0, 0, 0, 1) + mode(2, 1, 0, 0),
        mode(1, 0, 0, 1) + mode(2, 0, 1, 0),
        mode(0, 0, 1, 0) + mode(1, 1, 0, 0),
    ]
    bent = [
        (mode(1, 0, 1, 1), mode(0, 1, 0, 1)),
        (mode(2, 0, 1, 1), mode(0, 1, 1, 0)),
        (mode(2, 1, 0, 1), mode(1, 1, 1, 0)),
    ]
    twisted = [mode(0, 0, 1, 1), mode(1, 1, 0, 1), mode(2, 1, 1, 0)]
    warped = [mode(0, 1, 1, 1), mode(1, 1, 1, 1), mode(2, 1, 1, 1)]
    main = 2.0 * (square(normal[0]) + square(normal[1]) + square(normal[2]))
    main = main + (square(sheared[0]) + square(sheared[1]) + square(sheared[2]))
    half = None
    for left, right in bent:
        main = main + (square(left) + square(right))
        term = square(left + right)
        half = term if half is None else half + term
    main = main + 0.5 * half
    twists = square(twisted[0]) + square(twisted[1]) + square(twisted[2])
    twists = twists + square(twisted[0] + twisted[1] + twisted[2])
    warps = square(warped[0]) + square(warped[1]) + square(warped[2])
    return (shear * main + bulk * square(trace)) + (twist * twists + warp * warps)


def flag(condition):
    return jnp.where(condition, 1.0, 0.0).astype(jnp.float32)


def y_flags():
    rank = lax.axis_index("gy")
    return flag(rank > 0), flag(rank < lax.axis_size("gy") - 1)


def edge_rows(first, last, side):
    if side == "first":
        return first[0:SLOT]
    moved_up = pltpu.roll(last, SLOT, 0)
    if side == "last":
        return moved_up[0:SLOT]
    return jnp.where(lax.axis_index("gy") == 0, moved_up, first)[0:SLOT]


def layer_kernel(displacement, fixed, out):
    free = (1 - fixed[0]).astype(jnp.float32)
    for component in range(3):
        out[component] = displacement[0, component, 0] * free


def edge_kernel(sides, layers, *refs):
    (u_first, u_last, f_first, f_last, d_first, d_last, v_first, v_last, d_low, d_high) = refs[:10]
    outs = refs[10:]
    core = lax.axis_index("lc")
    outs[0][...] = jnp.where(core == 0, d_low[...], d_high[...])
    for number, side in enumerate(sides):
        packed, node_corner, design_corner = outs[1 + 3 * number : 4 + 3 * number]
        low, high = [], []
        for layer in range(layers):
            free = edge_rows(
                (1 - f_first[layer]).astype(jnp.float32),
                (1 - f_last[layer]).astype(jnp.float32),
                side,
            )
            for component in range(3):
                moved = free * edge_rows(u_first[0, component, layer], u_last[0, component, layer], side)
                packed[component * layers + layer] = moved
                if layer == 0:
                    node_corner[component] = moved
            design = edge_rows(d_first[layer], d_last[layer], side)
            packed[3 * layers + layer] = design
            if layer < 2:
                low.append(design)
            if layer >= layers - 2:
                high.append(design)
            packed[4 * layers + layer] = edge_rows(
                (1 - v_first[layer]).astype(jnp.float32),
                (1 - v_last[layer]).astype(jnp.float32),
                side,
            )
        for index in range(2):
            design_corner[index] = jnp.where(core == 0, low[index], high[index])


def energy_kernel(count, displacement, fixed, ratio, above, *refs):
    halos, corners = refs[:count], refs[count : 2 * count]
    mine, theirs, nodes, energy = refs[2 * count :]
    layers, rows, depth = fixed.shape
    core = lax.axis_index("lc")
    has_left, has_right = y_flags()
    zero_tile = filled((TILE, depth))
    for component in range(3):
        for layer in range(layers + 1):
            if layer < layers:
                free = (1 - fixed[layer]).astype(jnp.float32)
                nodes[component, layer, TILE : TILE + rows, :] = displacement[0, component, layer] * free
                left, right = (halo[component * layers + layer] for halo in (halos[0], halos[-1]))
            else:
                nodes[component, layer, TILE : TILE + rows, :] = above[component]
                left, right = (corner[component] for corner in (corners[0], corners[-1]))
            nodes[component, layer, 0:TILE, :] = zero_tile
            nodes[component, layer, TILE - SLOT : TILE, :] = left * has_left
            nodes[component, layer, TILE + rows : 2 * TILE + rows, :] = zero_tile
            nodes[component, layer, 2 * TILE + rows : 3 * TILE + rows, :] = zero_tile
            nodes[component, layer, TILE + rows : TILE + rows + SLOT, :] = right * has_right
    total = ratio[0]
    for case in range(1, ratio.shape[0]):
        total = total + ratio[case]
    share = filled((TILE, depth), ratio[core].astype(jnp.float32)) / filled((TILE, depth), total.astype(jnp.float32))
    for row in range(0, rows + 2 * TILE, TILE):
        lower = node_modes(nodes, 0, row)
        for layer in range(layers):
            upper = node_modes(nodes, layer + 1, row)
            energy[layer, row : row + TILE, :] = share * element_energy(lower, upper)
            lower = upper
    half = layers // 2
    mine[...] = energy[pl.ds(core * half, half)]
    theirs[...] = energy[pl.ds((1 - core) * half, half)]


def scaling_kernel(count, density, void, beyond, *refs):
    halos, corners = refs[:count], refs[count : 2 * count]
    scaling, design = refs[2 * count :]
    layers, rows, depth = density.shape
    half = layers // 2
    core = lax.axis_index("lc")
    has_left, has_right = y_flags()
    start = core * half
    zero_tile = filled((TILE, depth))
    origin = 2 * TILE

    def place(slot, middle, left, right):
        design[slot, 0:TILE, :] = zero_tile
        design[slot, TILE : 2 * TILE, :] = zero_tile
        design[slot, origin - SLOT : origin, :] = left * has_left
        design[slot, origin : origin + rows, :] = middle
        design[slot, origin + rows : origin + rows + TILE, :] = zero_tile
        design[slot, origin + rows + TILE : origin + rows + 2 * TILE, :] = zero_tile
        design[slot, origin + rows : origin + rows + SLOT, :] = right * has_right

    for index in range(half + 2):
        source = index + core * (half - 2)
        place(
            index + 2 * (1 - core),
            density[source],
            halos[0][3 * layers + source],
            halos[-1][3 * layers + source],
        )
    for index in range(2):
        place(core * (half + 2) + index, beyond[index], corners[0][index], corners[-1][index])

    total_x = layers * lax.axis_size("gz")
    total_y = rows * lax.axis_size("gy")
    first_layer = lax.axis_index("gz") * layers + start
    first_row = lax.axis_index("gy") * rows
    lane = lax.broadcasted_iota(jnp.int32, (TILE, depth), 1)
    count1 = jnp.where((lane == 0) | (lane == depth - 1), 1.0, 2.0)
    count2 = jnp.where((lane < 2) | (lane >= depth - 2), 1.0, 2.0)
    for row in range(0, rows + 2 * TILE, TILE):
        column = lax.broadcasted_iota(jnp.int32, (TILE, 128), 0) + (first_row + row - TILE)

        def within(offset):
            at = column + offset
            return jnp.where((at >= 0) & (at < total_y), 1.0, 0.0)

        y0, y1, y2 = within(0), within(-1) + within(1), within(-2) + within(2)
        for layer, filtered in cone_rows(design, row + TILE, half):
            at = first_layer + layer

            def inside(offset):
                return flag((at + offset >= 0) & (at + offset < total_x))

            x1 = inside(-1) + inside(1)
            x2 = inside(-2) + inside(2)
            levels = depth_levels(y0, x1 * y0 + y1, x1 * y1, x2 * y0 + y2, x1 * y2 + x2 * y1)
            level0, level1, level2 = (
                jnp.concatenate([level] * (depth // 128), axis=1) for level in levels
            )
            weight_sum = jnp.maximum(level0 + count1 * level1 + count2 * level2, 1.0)
            inverse = 1.0 / weight_sum
            physical = filtered * inverse
            value = (-3.0 * (1.0 - 0.001)) * physical * physical * inverse
            if row == 0:
                alive = has_left * halos[0][4 * layers + start + layer]
                scaling[layer, 0:TILE, :] = zero_tile
                scaling[layer, TILE - SLOT : TILE, :] = value[TILE - SLOT :] * alive
            elif row == rows + TILE:
                alive = has_right * halos[-1][4 * layers + start + layer]
                scaling[layer, row : row + TILE, :] = zero_tile
                scaling[layer, row : row + SLOT, :] = value[0:SLOT] * alive
            else:
                alive = (1 - void[start + layer, row - TILE : row, :]).astype(jnp.float32)
                scaling[layer, row : row + TILE, :] = value * alive


def sensed_kernel(scaling, mine, received, sensed, outgoing):
    half = scaling.shape[0]
    core = lax.axis_index("lc")
    for layer in range(half):
        sensed[layer] = scaling[layer] * (mine[layer] + received[layer])
    outgoing[...] = sensed[pl.ds(core * (half - 2), 2)]


def gradient_kernel(void, own, other, own_beyond, other_beyond, gradient, field):
    layers, rows, depth = void.shape
    half = layers // 2
    core = lax.axis_index("lc")
    field[pl.ds(2 + core * half, half)] = own[...]
    field[pl.ds(2 + (1 - core) * half, half)] = other[...]
    field[pl.ds(core * (layers + 2), 2)] = own_beyond[...]
    field[pl.ds((1 - core) * (layers + 2), 2)] = other_beyond[...]
    for row in range(TILE, TILE + rows, TILE):
        for layer, filtered in cone_rows(field, row, layers):
            alive = (1 - void[layer, row - TILE : row, :]).astype(jnp.float32)
            gradient[layer, row - TILE : row, :] = alive * filtered


def call(kernel, outs, scratch, flops, name, **more):
    return pl.pallas_call(
        kernel,
        out_shape=[jax.ShapeDtypeStruct(shape, jnp.float32) for shape in outs],
        scratch_shapes=[pltpu.VMEM(shape, jnp.float32) for shape in scratch],
        cost_estimate=pl.CostEstimate(flops=flops, bytes_accessed=1 << 20, transcendentals=0),
        compiler_params=pltpu.CompilerParams(vmem_limit_bytes=24 << 20),
        name=name,
        **more,
    )


def whole():
    return pl.BlockSpec(memory_space=pltpu.VMEM)


def shards(density, void_mask, fixed_mask, displacement, load_ratio):
    layers, rows, depth = density.shape
    half = layers // 2
    wide = rows + 2 * TILE
    gz, gy, lc = (lax.axis_size(axis) for axis in ("gz", "gy", "lc"))
    swap = [(0, 1), (1, 0)]
    down = [(z, z - 1) for z in range(1, gz)]
    split = []
    for z in range(gz):
        if z > 0:
            split.append((z * lc, (z - 1) * lc + 1))
        if z < gz - 1:
            split.append((z * lc + 1, (z + 1) * lc))

    def y_pairs(step):
        if gy == 2:
            return [(y, 1 - y) for y in range(gy)]
        return [(y, y + step) for y in range(gy) if 0 <= y + step < gy]

    def node_corner_pairs(step):
        return [(z * gy + y, (z - 1) * gy + peer) for z in range(1, gz) for y, peer in y_pairs(step)]

    def design_corner_pairs(step):
        return [
            ((a // lc * gy + y) * lc + a % lc, (b // lc * gy + peer) * lc + b % lc)
            for a, b in split
            for y, peer in y_pairs(step)
        ]

    block_rows = rows // TILE - 1
    first_u = pl.BlockSpec((1, 3, layers, TILE, depth), lambda i: (0, 0, 0, 0, 0))
    last_u = pl.BlockSpec((1, 3, layers, TILE, depth), lambda i: (0, 0, 0, block_rows, 0))
    first_s = pl.BlockSpec((layers, TILE, depth), lambda i: (0, 0, 0))
    last_s = pl.BlockSpec((layers, TILE, depth), lambda i: (0, block_rows, 0))
    low_s = pl.BlockSpec((2, rows, depth), lambda i: (0, 0, 0))
    high_s = pl.BlockSpec((2, rows, depth), lambda i: (layers // 2 - 1, 0, 0))
    sides = ["both"] if gy == 2 else ["first", "last"]

    (layer_out,) = call(
        layer_kernel,
        [(3, rows, depth)],
        [],
        1 << 18,
        "layer",
        grid=(1,),
        in_specs=[
            pl.BlockSpec((1, 3, 1, rows, depth), lambda i: (0, 0, 0, 0, 0)),
            pl.BlockSpec((1, rows, depth), lambda i: (0, 0, 0)),
        ],
        out_specs=[pl.BlockSpec((3, rows, depth), lambda i: (0, 0, 0))],
    )(displacement, fixed_mask)
    above = lax.ppermute(layer_out, "gz", down)

    out_shapes = [(2, rows, depth)]
    for _ in sides:
        out_shapes += [(5 * layers, SLOT, depth), (3, SLOT, depth), (2, SLOT, depth)]
    edges = call(
        functools.partial(edge_kernel, sides, layers),
        out_shapes,
        [],
        1 << 20,
        "edge",
        grid=(1,),
        in_specs=[first_u, last_u, first_s, last_s, first_s, last_s, first_s, last_s, low_s, high_s],
        out_specs=[pl.BlockSpec(shape, lambda i: (0, 0, 0)) for shape in out_shapes],
    )(
        displacement, displacement, fixed_mask, fixed_mask, density, density,
        void_mask, void_mask, density, density,
    )
    design_out, edges = edges[0], edges[1:]
    packs, node_corners, design_corners = edges[0::3], edges[1::3], edges[2::3]
    steps = [1] if gy == 2 else [-1, 1]
    halos = [lax.ppermute(pack, "gy", y_pairs(step)) for pack, step in zip(packs, steps)]
    corners = [
        lax.ppermute(corner, ("gz", "gy"), node_corner_pairs(step))
        for corner, step in zip(node_corners, steps)
    ]
    beyond = lax.ppermute(design_out, ("gz", "lc"), split)
    outer = [
        lax.ppermute(corner, ("gz", "gy", "lc"), design_corner_pairs(step))
        for corner, step in zip(design_corners, steps)
    ]
    halos, corners, outer = halos[::-1], corners[::-1], outer[::-1]
    count = len(sides)

    (scaling,) = call(
        functools.partial(scaling_kernel, count),
        [(half, wide, depth)],
        [(half + 4, wide + 2 * TILE, depth)],
        1 << 22,
        "scaling",
        in_specs=[whole()] * (3 + 2 * count),
        out_specs=[whole()],
    )(density, void_mask, beyond, *halos, *outer)
    mine, theirs = call(
        functools.partial(energy_kernel, count),
        [(half, wide, depth)] * 2,
        [(3, layers + 1, wide + TILE, depth), (layers, wide, depth)],
        1 << 24,
        "energy",
        in_specs=[whole(), whole(), pl.BlockSpec(memory_space=pltpu.SMEM)] + [whole()] * (1 + 2 * count),
        out_specs=[whole()] * 2,
    )(displacement, fixed_mask, load_ratio, above, *halos, *corners)
    received = lax.ppermute(theirs, "lc", swap)
    sensed, outgoing = call(
        sensed_kernel,
        [(half, wide, depth), (2, wide, depth)],
        [],
        1 << 20,
        "sensed",
        in_specs=[whole()] * 3,
        out_specs=[whole()] * 2,
    )(scaling, mine, received)
    own_beyond = lax.ppermute(outgoing, ("gz", "lc"), split)
    other = lax.ppermute(sensed, "lc", swap)
    other_beyond = lax.ppermute(own_beyond, "lc", swap)
    (gradient,) = call(
        gradient_kernel,
        [(layers, rows, depth)],
        [(layers + 4, wide, depth)],
        1 << 23,
        "gradient",
        in_specs=[whole()] * 5,
        out_specs=[whole()],
    )(void_mask, sensed, other, own_beyond, other_beyond)
    return gradient


def solution(mesh):
    placed = (
        P(("parts", "gz"), "gy", None),
        P(("parts", "gz"), "gy", None),
        P(("parts", "gz"), "gy", None),
        P("lc", None, ("parts", "gz"), "gy", None),
        P("parts"),
    )
    return jax.shard_map(
        shards,
        mesh=mesh,
        in_specs=placed,
        out_specs=P(("parts", "gz"), "gy", None),
        check_vma=False,
    )
```

```python
import functools
import math

import jax
import jax.numpy as jnp
from jax import lax
from jax.experimental import pallas as pl
from jax.experimental.pallas import tpu as pltpu
from jax.sharding import PartitionSpec as P

TILE = 8
SLOT = 4
LANES = 128
VMEM_BYTES = 67043328
WEIGHT = [2.5 - math.sqrt(squared) for squared in range(7)]


def energy_factors():
    poisson = 0.3
    factor = 1.0 / ((1.0 + poisson) * (1.0 - 2.0 * poisson))
    shear = factor * (0.5 - poisson) / 16.0
    bulk = factor * poisson / 16.0
    twist = factor * (0.5 - poisson) / 48.0
    warp = factor * ((1.0 - poisson) + 2.0 * (0.5 - poisson)) / 144.0
    return shear, bulk, twist, warp


def filled(shape, value=0.0):
    return jnp.full(shape, value, jnp.float32)


def lane_index():
    return lax.broadcasted_iota(jnp.int32, (TILE, LANES), 1)


def row_index():
    return lax.broadcasted_iota(jnp.int32, (TILE, LANES), 0)


def parts_of(depth):
    return [slice(at, at + LANES) for at in range(0, depth, LANES)]


def along_depth(values, offset):
    lane = lane_index()
    turned = [pltpu.roll(value, (-offset) % LANES, 1) for value in values]
    zero = filled((TILE, LANES))
    if offset > 0:
        keep, beyond = lane < LANES - offset, turned[1:] + [zero]
    else:
        keep, beyond = lane >= -offset, [zero] + turned[:-1]
    return [jnp.where(keep, own, other) for own, other in zip(turned, beyond)]


def along_rows(tiles, offset):
    turned = [pltpu.roll(tile, (-offset) % TILE, 0) for tile in tiles]
    if offset > 0:
        keep, beyond = row_index() < TILE - offset, turned[1:] + turned[:1]
    else:
        keep, beyond = row_index() >= -offset, turned[-1:] + turned[:-1]
    return [jnp.where(keep, own, other) for own, other in zip(turned, beyond)]


def row_sums(source, sums, layers, wide):
    depth = source.shape[-1]
    for layer in layers:
        for part in parts_of(depth):
            tiles = [source[layer, row : row + TILE, part] for row in range(0, wide, TILE)]
            for number, distance in enumerate((1, 2)):
                ahead, behind = along_rows(tiles, distance), along_rows(tiles, -distance)
                for index, (one, other) in enumerate(zip(ahead, behind)):
                    sums[layer, number, TILE * index : TILE * (index + 1), part] = one + other


def depth_levels(plain, near, corner, far, knight):
    w = WEIGHT
    level0 = w[0] * plain + w[1] * near + w[2] * corner + w[4] * far + w[5] * knight
    level1 = w[1] * plain + w[2] * near + w[3] * corner + w[5] * far + w[6] * knight
    level2 = w[4] * plain + w[5] * near + w[6] * corner
    return level0, level1, level2


def cone_tile(source, sums, layer, row):
    results = []
    for part in parts_of(source.shape[-1]):

        def plane(at):
            return source[layer + at, row : row + TILE, part]

        def summed(at, number):
            return sums[layer + at, number, row : row + TILE, part]

        near = (plane(-1) + plane(1)) + summed(0, 0)
        corner = summed(-1, 0) + summed(1, 0)
        far = (plane(-2) + plane(2)) + summed(0, 1)
        knight = (summed(-1, 1) + summed(1, 1)) + (summed(-2, 0) + summed(2, 0))
        results.append(depth_levels(plane(0), near, corner, far, knight))
    level1 = [levels[1] for levels in results]
    level2 = [levels[2] for levels in results]
    shifted = [along_depth(level1, 1), along_depth(level1, -1), along_depth(level2, 2), along_depth(level2, -2)]
    return [
        levels[0] + ((one + two) + (three + four))
        for levels, one, two, three, four in zip(results, *shifted)
    ]


def row_modes(nodes, modes, layer, slot, wide):
    for component in range(3):
        for part in parts_of(nodes.shape[-1]):
            tiles = [nodes[component, layer, row : row + TILE, part] for row in range(0, wide, TILE)]
            for index, (low, high) in enumerate(zip(tiles, along_rows(tiles, 1))):
                at = slice(TILE * index, TILE * (index + 1))
                modes[slot, 2 * component, at, part] = low + high
                modes[slot, 2 * component + 1, at, part] = high - low


def node_modes(modes, slot, row):
    parts = parts_of(modes.shape[-1])
    found = [[] for _ in parts]
    for number in range(6):
        values = [modes[slot, number, row : row + TILE, part] for part in parts]
        for mine, value, after in zip(found, values, along_depth(values, 1)):
            mine.append(value + after)
            mine.append(after - value)
    return found


def element_energy(lower, upper, scale):
    def mode(component, first, second, third):
        index = 4 * component + 2 * second + third
        if first:
            return upper[index] - lower[index]
        return upper[index] + lower[index]

    def square(value):
        return value * value

    normal = [mode(0, 1, 0, 0), mode(1, 0, 1, 0), mode(2, 0, 0, 1)]
    trace = normal[0] + normal[1] + normal[2]
    main = square(mode(0, 0, 0, 1) + mode(2, 1, 0, 0))
    main = main + square(mode(1, 0, 0, 1) + mode(2, 0, 1, 0))
    main = main + square(mode(0, 0, 1, 0) + mode(1, 1, 0, 0))
    bent = [
        (mode(1, 0, 1, 1), mode(0, 1, 0, 1)),
        (mode(2, 0, 1, 1), mode(0, 1, 1, 0)),
        (mode(2, 1, 0, 1), mode(1, 1, 1, 0)),
    ]
    half = None
    for left, right in bent:
        main = main + square(left + right)
        term = square(left - right)
        half = term if half is None else half + term
    main = main + 2.0 * (square(normal[0]) + square(normal[1]) + square(normal[2]))
    main = main + 0.5 * half
    twisted = [mode(0, 0, 1, 1), mode(1, 1, 0, 1), mode(2, 1, 1, 0)]
    twists = square(twisted[0]) + square(twisted[1]) + square(twisted[2])
    twists = twists + square(twisted[0] + twisted[1] + twisted[2])
    warps = square(mode(0, 1, 1, 1)) + square(mode(1, 1, 1, 1)) + square(mode(2, 1, 1, 1))
    shear, bulk, twist, warp = scale
    return (shear * main + bulk * square(trace)) + (twist * twists + warp * warps)


def shares(ratio):
    total = ratio[0]
    for case in range(1, ratio.shape[0]):
        total = total + ratio[case]
    total = filled((TILE, LANES), total.astype(jnp.float32))

    def scale(case):
        share = filled((TILE, LANES), ratio[case].astype(jnp.float32)) / total
        return [factor * share for factor in energy_factors()]

    return scale


def flag(condition):
    return jnp.where(condition, 1.0, 0.0).astype(jnp.float32)


def y_flags():
    rank = lax.axis_index("gy")
    return flag(rank > 0), flag(rank < lax.axis_size("gy") - 1)


def free_of(mask):
    return (1 - mask).astype(jnp.float32)


def edge_rows(first, last, side):
    if side == "first":
        return first[0:SLOT]
    moved_up = pltpu.roll(last, SLOT, 0)
    if side == "last":
        return moved_up[0:SLOT]
    return jnp.where(lax.axis_index("gy") == 0, moved_up, first)[0:SLOT]


def layer_kernel(displacement, fixed, density, crossing, straight, nodes, mask, sems):
    layers = density.shape[0]
    core = lax.axis_index("lc")
    copies = [
        pltpu.make_async_copy(displacement.at[0, :, 0], nodes, sems.at[0]),
        pltpu.make_async_copy(fixed.at[0], mask, sems.at[1]),
        pltpu.make_async_copy(
            density.at[pl.ds(core * (layers - 2), 2)], crossing.at[pl.ds(3, 2)], sems.at[2]
        ),
    ]
    for copy in copies:
        copy.start()
    for copy in copies:
        copy.wait()
    free = free_of(mask[...])
    for component in range(3):
        moved = nodes[component] * free
        crossing[component] = moved
        straight[component] = moved


def edge_kernel(sides, displacement, fixed, density, void, *outs):
    layers, rows, _ = density.shape
    core = lax.axis_index("lc")
    first, last = slice(0, TILE), slice(rows - TILE, rows)
    for number, side in enumerate(sides):
        packed, crossing, straight = outs[3 * number : 3 * number + 3]
        low, high = [], []
        for layer in range(layers):
            free = edge_rows(free_of(fixed[layer, first]), free_of(fixed[layer, last]), side)
            for component in range(3):
                moved = free * edge_rows(
                    displacement[0, component, layer, first], displacement[0, component, layer, last], side
                )
                packed[component * layers + layer] = moved
                if layer == 0:
                    crossing[component] = moved
                    straight[component] = moved
            design = edge_rows(density[layer, first], density[layer, last], side)
            packed[3 * layers + layer] = design
            if layer < 2:
                low.append(design)
            if layer >= layers - 2:
                high.append(design)
            packed[4 * layers + layer] = edge_rows(
                free_of(void[layer, first]), free_of(void[layer, last]), side
            )
        for index in range(2):
            crossing[3 + index] = jnp.where(core == 0, low[index], high[index])


def energy_kernel(count, displacement, fixed, ratio, *refs):
    halos = refs[:count]
    mine, theirs, last, nodes, modes, energy = refs[count:]
    layers, rows, depth = fixed.shape
    wide = rows + TILE
    half = layers // 2
    core = lax.axis_index("lc")
    has_left, has_right = y_flags()
    for layer in range(layers):
        free = free_of(fixed[layer])
        for component in range(3):
            nodes[component, layer, 0:rows, :] = displacement[0, component, layer] * free
            at = component * layers + layer
            nodes[component, layer, rows : rows + SLOT, :] = halos[-1][at] * has_right
            nodes[component, layer, rows + SLOT : wide, :] = halos[0][at] * has_left
        row_modes(nodes, modes, layer, layer, wide)
    scale = shares(ratio)(core)
    for row in range(0, wide, TILE):
        lower = node_modes(modes, 0, row)
        for layer in range(layers - 1):
            upper = node_modes(modes, layer + 1, row)
            for part, below, above in zip(parts_of(depth), lower, upper):
                energy[layer, row : row + TILE, part] = element_energy(below, above, scale)
            lower = upper
    for component in range(3):
        last[component] = nodes[component, layers - 1]
    mine[0 : half - 1] = energy[pl.ds(core * half, half - 1)]

    @pl.when(core == 0)
    def _():
        mine[half - 1] = energy[half - 1]
        theirs[0 : half - 1] = energy[half : layers - 1]
        theirs[half : half + 3] = nodes[:, layers - 1]

    @pl.when(core == 1)
    def _():
        theirs[0:half] = energy[0:half]


def scaling_kernel(count, density, void, beyond, *refs):
    halos, corners = refs[:count], refs[count : 2 * count]
    scaling, design, sums, halo_alive = refs[2 * count :]
    layers, rows, depth = density.shape
    wide = rows + TILE
    half = layers // 2
    core = lax.axis_index("lc")
    has_left, has_right = y_flags()
    start = core * half

    def place(slot, middle, left, right):
        design[slot, 0:rows, :] = middle
        design[slot, rows : rows + SLOT, :] = right * has_right
        design[slot, rows + SLOT : wide, :] = left * has_left

    for index in range(half + 2):
        source = index + core * (half - 2)
        at = 3 * layers + source
        place(index + 2 * (1 - core), density[source], halos[0][at], halos[-1][at])
    for index in range(2):
        place(core * (half + 2) + index, beyond[3 + index], corners[0][3 + index], corners[-1][3 + index])
    for layer in range(half):
        at = 4 * layers + start + layer
        halo_alive[layer, 0:SLOT, :] = halos[-1][at] * has_right
        halo_alive[layer, SLOT:TILE, :] = halos[0][at] * has_left
    row_sums(design, sums, range(half + 4), wide)

    total_x = layers * lax.axis_size("gz")
    total_y = rows * lax.axis_size("gy")
    first_layer = lax.axis_index("gz") * layers + start
    first_row = lax.axis_index("gy") * rows
    parts = parts_of(depth)
    lane = lane_index()

    def depth_count(number, distance):
        held = filled((TILE, LANES), 2.0)
        if number == 0:
            held = jnp.where(lane < distance, 1.0, held)
        if number == len(parts) - 1:
            held = jnp.where(lane >= LANES - distance, held - 1.0, held)
        return held

    counts = [(depth_count(number, 1), depth_count(number, 2)) for number in range(len(parts))]

    def inside(at):
        return flag((at >= 0) & (at < total_x))

    for row in range(0, wide, TILE):
        column = row_index() + (first_row + row)
        if row == rows:
            column = jnp.where(row_index() >= SLOT, column - (rows + TILE), column)

        def within(offset):
            at = column + offset
            return jnp.where((at >= 0) & (at < total_y), 1.0, 0.0)

        y0, y1, y2 = within(0), within(-1) + within(1), within(-2) + within(2)
        for layer in range(half):
            filtered = cone_tile(design, sums, layer + 2, row)
            at = first_layer + layer
            x1 = inside(at - 1) + inside(at + 1)
            x2 = inside(at - 2) + inside(at + 2)
            level0, level1, level2 = depth_levels(
                y0, x1 * y0 + y1, x1 * y1, x2 * y0 + y2, x1 * y2 + x2 * y1
            )
            for part, value, (count1, count2) in zip(parts, filtered, counts):
                weight_sum = jnp.maximum(level0 + count1 * level1 + count2 * level2, 1.0)
                inverse = 1.0 / weight_sum
                physical = value * inverse
                value = (-3.0 * (1.0 - 0.001)) * physical * physical * inverse
                if row == rows:
                    alive = halo_alive[layer, :, part]
                else:
                    alive = free_of(void[start + layer, row : row + TILE, part])
                scaling[layer, row : row + TILE, part] = value * alive


def sensed_kernel(count, scaling, mine, received, last, ratio, crossing, straight, *refs):
    crossing_corners, straight_corners = refs[:count], refs[count : 2 * count]
    sensed, outgoing, nodes, modes = refs[2 * count :]
    half, wide, depth = scaling.shape
    rows = wide - TILE
    core = lax.axis_index("lc")
    for layer in range(half - 1):
        sensed[layer] = scaling[layer] * (mine[layer] + received[layer])

    @pl.when(core == 0)
    def _():
        sensed[half - 1] = scaling[half - 1] * (mine[half - 1] + received[half - 1])
        outgoing[...] = sensed[0:2]

    @pl.when(core == 1)
    def _():
        has_left, has_right = y_flags()
        scales = shares(ratio)
        cases = ((crossing, crossing_corners), (straight, straight_corners))
        for case, (above, corners) in enumerate(cases):
            for component in range(3):
                if case == 0:
                    nodes[component, 2 * case] = received[half + component]
                else:
                    nodes[component, 2 * case] = last[component]
                nodes[component, 2 * case + 1, 0:rows, :] = above[component]
                nodes[component, 2 * case + 1, rows : rows + SLOT, :] = corners[-1][component] * has_right
                nodes[component, 2 * case + 1, rows + SLOT : wide, :] = corners[0][component] * has_left
            for index in (2 * case, 2 * case + 1):
                row_modes(nodes, modes, index, index, wide)
        for row in range(0, wide, TILE):
            totals = None
            for case in range(2):
                lower, upper = (node_modes(modes, 2 * case + side, row) for side in (0, 1))
                energies = [element_energy(a, b, scales(case)) for a, b in zip(lower, upper)]
                totals = energies if totals is None else [a + b for a, b in zip(totals, energies)]
            for part, value in zip(parts_of(depth), totals):
                sensed[half - 1, row : row + TILE, part] = scaling[half - 1, row : row + TILE, part] * value
        outgoing[...] = sensed[half - 2 : half]


def inner_kernel(void, own, other, gradient, field, sums):
    layers, rows, depth = void.shape
    wide = rows + TILE
    half = layers // 2
    core = lax.axis_index("lc")
    field[pl.ds(core * half, half)] = own[...]
    field[pl.ds((1 - core) * half, half)] = other[...]
    row_sums(field, sums, range(layers), wide)
    for row in range(0, rows, TILE):
        for layer in range(2, layers - 2):
            filtered = cone_tile(field, sums, layer, row)
            for part, value in zip(parts_of(depth), filtered):
                alive = free_of(void[layer, row : row + TILE, part])
                gradient[layer - 2, row : row + TILE, part] = alive * value


def outer_kernel(void, own, other, own_beyond, other_beyond, inner, gradient, field, sums, low, high, sems):
    layers, rows, depth = void.shape
    wide = rows + TILE
    half = layers // 2
    core = lax.axis_index("lc")
    middle = pltpu.make_async_copy(inner, gradient.at[pl.ds(2, layers - 4)], sems.at[0])
    middle.start()
    field[pl.ds(2 + core * half, half)] = own[...]
    field[pl.ds(2 + (1 - core) * half, half)] = other[...]
    field[pl.ds(core * (layers + 2), 2)] = own_beyond[...]
    field[pl.ds((1 - core) * (layers + 2), 2)] = other_beyond[...]
    copies = [middle]
    for number, (result, base) in enumerate(((low, 0), (high, layers - 2))):
        row_sums(field, sums, range(base, base + 6), wide)
        for row in range(0, rows, TILE):
            for layer in range(2):
                filtered = cone_tile(field, sums, base + layer + 2, row)
                for part, value in zip(parts_of(depth), filtered):
                    alive = free_of(void[base + layer, row : row + TILE, part])
                    result[layer, row : row + TILE, part] = alive * value
        copy = pltpu.make_async_copy(result, gradient.at[pl.ds(base, 2)], sems.at[1 + number])
        copy.start()
        copies.append(copy)
    for copy in copies:
        copy.wait()


def vmem():
    return pl.BlockSpec(memory_space=pltpu.VMEM)


def hbm():
    return pl.BlockSpec(memory_space=pltpu.HBM)


def call(kernel, outs, scratch, in_specs, flops, out_specs=None, sems=0, limit=24 << 20):
    scratch = [pltpu.VMEM(shape, kind) for shape, kind in scratch]
    if sems:
        scratch.append(pltpu.SemaphoreType.DMA((sems,)))
    return pl.pallas_call(
        kernel,
        out_shape=[jax.ShapeDtypeStruct(shape, jnp.float32) for shape in outs],
        in_specs=in_specs,
        out_specs=out_specs or [vmem()] * len(outs),
        scratch_shapes=scratch,
        cost_estimate=pl.CostEstimate(flops=flops, bytes_accessed=1 << 20, transcendentals=0),
        compiler_params=pltpu.CompilerParams(vmem_limit_bytes=limit),
    )


def shards(density, void_mask, fixed_mask, displacement, load_ratio):
    layers, rows, depth = density.shape
    half = layers // 2
    wide = rows + TILE
    gz, gy, lc = (lax.axis_size(axis) for axis in ("gz", "gy", "lc"))
    real = jnp.float32
    smem = pl.BlockSpec(memory_space=pltpu.SMEM)
    swap = [(0, 1), (1, 0)]
    crossing, straight = [], []
    for z in range(1, gz):
        crossing.append((z * lc, (z - 1) * lc + 1))
        crossing.append(((z - 1) * lc + 1, z * lc))
        straight.append((z * lc + 1, (z - 1) * lc + 1))

    def y_pairs(step):
        if gy == 2:
            return [(y, 1 - y) for y in range(gy)]
        return [(y, y + step) for y in range(gy) if 0 <= y + step < gy]

    def diagonal(pairs, step):
        return [
            ((a // lc * gy + y) * lc + a % lc, (b // lc * gy + peer) * lc + b % lc)
            for a, b in pairs
            for y, peer in y_pairs(step)
        ]

    sides, steps = (["both"], [1]) if gy == 2 else (["first", "last"], [-1, 1])
    count = len(sides)

    crossing_out, straight_out = call(
        layer_kernel,
        [(5, rows, depth), (3, rows, depth)],
        [((3, rows, depth), real), ((rows, depth), jnp.int32)],
        [hbm()] * 3,
        1 << 18,
        sems=3,
        limit=VMEM_BYTES - 128 * rows * depth * 4,
    )(displacement, fixed_mask, density)
    crossed = lax.ppermute(crossing_out, ("gz", "lc"), crossing)
    straightened = lax.ppermute(straight_out, ("gz", "lc"), straight)
    density, void_mask, fixed_mask, displacement, crossing_out = lax.optimization_barrier(
        (density, void_mask, fixed_mask, displacement, crossing_out)
    )
    edges = call(
        functools.partial(edge_kernel, sides),
        [(5 * layers, SLOT, depth), (5, SLOT, depth), (3, SLOT, depth)] * count,
        [],
        [vmem()] * 4,
        1 << 20,
    )(displacement, fixed_mask, density, void_mask)
    halos = [lax.ppermute(a, "gy", y_pairs(step)) for a, step in zip(edges[0::3], steps)][::-1]
    axes = ("gz", "gy", "lc")
    crossed_corners = [lax.ppermute(a, axes, diagonal(crossing, step)) for a, step in zip(edges[1::3], steps)][::-1]
    straight_corners = [lax.ppermute(a, axes, diagonal(straight, step)) for a, step in zip(edges[2::3], steps)][::-1]

    mine, theirs, last = call(
        functools.partial(energy_kernel, count),
        [(half, wide, depth), (half + 3, wide, depth), (3, wide, depth)],
        [((3, layers, wide, depth), real), ((layers, 6, wide, depth), real), ((layers, wide, depth), real)],
        [vmem(), vmem(), smem] + [vmem()] * count,
        1 << 24,
    )(displacement, fixed_mask, load_ratio, *halos)
    received = lax.ppermute(theirs, "lc", swap)
    (scaling,) = call(
        functools.partial(scaling_kernel, count),
        [(half, wide, depth)],
        [((half + 4, wide, depth), real), ((half + 4, 2, wide, depth), real), ((half, TILE, depth), real)],
        [vmem()] * (3 + 2 * count),
        1 << 22,
    )(density, void_mask, crossed, *halos, *crossed_corners)
    sensed, outgoing = call(
        functools.partial(sensed_kernel, count),
        [(half, wide, depth), (2, wide, depth)],
        [((3, 4, wide, depth), real), ((4, 6, wide, depth), real)],
        [vmem()] * 4 + [smem] + [vmem()] * (2 + 2 * count),
        1 << 22,
    )(scaling, mine, received, last, load_ratio, crossed, straightened, *crossed_corners, *straight_corners)
    own_beyond = lax.ppermute(outgoing, ("gz", "lc"), crossing)
    other = lax.ppermute(sensed, "lc", swap)
    (inner,) = call(
        inner_kernel,
        [(layers - 4, rows, depth)],
        [((layers, wide, depth), real), ((layers, 2, wide, depth), real)],
        [vmem()] * 3,
        1 << 22,
    )(void_mask, sensed, other)
    other_beyond = lax.ppermute(own_beyond, "lc", swap)
    (gradient,) = call(
        outer_kernel,
        [(layers, rows, depth)],
        [
            ((layers + 4, wide, depth), real),
            ((layers + 4, 2, wide, depth), real),
            ((2, rows, depth), real),
            ((2, rows, depth), real),
        ],
        [vmem()] * 6,
        1 << 22,
        out_specs=[hbm()],
        sems=3,
    )(void_mask, sensed, other, own_beyond, other_beyond, inner)
    return gradient


def solution(mesh):
    placed = (
        P(("parts", "gz"), "gy", None),
        P(("parts", "gz"), "gy", None),
        P(("parts", "gz"), "gy", None),
        P("lc", None, ("parts", "gz"), "gy", None),
        P("parts"),
    )
    return jax.shard_map(
        shards,
        mesh=mesh,
        in_specs=placed,
        out_specs=P(("parts", "gz"), "gy", None),
        check_vma=False,
    )
```

```python
import functools
import math

import jax
import jax.numpy as jnp
from jax import lax
from jax.experimental import pallas as pl
from jax.experimental.pallas import tpu as pltpu
from jax.sharding import PartitionSpec as P

TILE = 8
SLOT = 4
LANES = 128
PREPARE_LIMIT = 53 << 20
WEIGHT = [2.5 - math.sqrt(squared) for squared in range(7)]


def energy_factors():
    poisson = 0.3
    factor = 1.0 / ((1.0 + poisson) * (1.0 - 2.0 * poisson))
    shear = factor * (0.5 - poisson) / 16.0
    bulk = factor * poisson / 16.0
    twist = factor * (0.5 - poisson) / 48.0
    warp = factor * ((1.0 - poisson) + 2.0 * (0.5 - poisson)) / 144.0
    return shear, bulk, twist, warp


def filled(shape, value=0.0):
    return jnp.full(shape, value, jnp.float32)


def lane_index():
    return lax.broadcasted_iota(jnp.int32, (TILE, LANES), 1)


def row_index():
    return lax.broadcasted_iota(jnp.int32, (TILE, LANES), 0)


def parts_of(depth):
    return [slice(at, at + LANES) for at in range(0, depth, LANES)]


def along_depth(values, offset):
    lane = lane_index()
    turned = [pltpu.roll(value, (-offset) % LANES, 1) for value in values]
    zero = filled((TILE, LANES))
    if offset > 0:
        keep, beyond = lane < LANES - offset, turned[1:] + [zero]
    else:
        keep, beyond = lane >= -offset, [zero] + turned[:-1]
    return [jnp.where(keep, own, other) for own, other in zip(turned, beyond)]


def along_rows(tiles, offset):
    turned = [pltpu.roll(tile, (-offset) % TILE, 0) for tile in tiles]
    if offset > 0:
        keep, beyond = row_index() < TILE - offset, turned[1:] + turned[:1]
    else:
        keep, beyond = row_index() >= -offset, turned[-1:] + turned[:-1]
    return [jnp.where(keep, own, other) for own, other in zip(turned, beyond)]


def row_sums(source, sums, layers, wide):
    depth = source.shape[-1]
    for layer in layers:
        for part in parts_of(depth):
            tiles = [source[layer, row : row + TILE, part] for row in range(0, wide, TILE)]
            for number, distance in enumerate((1, 2)):
                ahead, behind = along_rows(tiles, distance), along_rows(tiles, -distance)
                for index, (one, other) in enumerate(zip(ahead, behind)):
                    sums[layer, number, TILE * index : TILE * (index + 1), part] = one + other


def depth_levels(plain, near, corner, far, knight):
    w = WEIGHT
    level0 = w[0] * plain + w[1] * near + w[2] * corner + w[4] * far + w[5] * knight
    level1 = w[1] * plain + w[2] * near + w[3] * corner + w[5] * far + w[6] * knight
    level2 = w[4] * plain + w[5] * near + w[6] * corner
    return level0, level1, level2


def cone_tile(source, sums, layer, row):
    results = []
    for part in parts_of(source.shape[-1]):

        def plane(at):
            return source[layer + at, row : row + TILE, part]

        def summed(at, number):
            return sums[layer + at, number, row : row + TILE, part]

        near = (plane(-1) + plane(1)) + summed(0, 0)
        corner = summed(-1, 0) + summed(1, 0)
        far = (plane(-2) + plane(2)) + summed(0, 1)
        knight = (summed(-1, 1) + summed(1, 1)) + (summed(-2, 0) + summed(2, 0))
        results.append(depth_levels(plane(0), near, corner, far, knight))
    level1 = [levels[1] for levels in results]
    level2 = [levels[2] for levels in results]
    shifted = [along_depth(level1, 1), along_depth(level1, -1), along_depth(level2, 2), along_depth(level2, -2)]
    return [
        levels[0] + ((one + two) + (three + four))
        for levels, one, two, three, four in zip(results, *shifted)
    ]


def row_modes(nodes, modes, layer, slot, wide):
    for component in range(3):
        for part in parts_of(nodes.shape[-1]):
            tiles = [nodes[component, layer, row : row + TILE, part] for row in range(0, wide, TILE)]
            for index, (low, high) in enumerate(zip(tiles, along_rows(tiles, 1))):
                at = slice(TILE * index, TILE * (index + 1))
                modes[slot, 2 * component, at, part] = low + high
                modes[slot, 2 * component + 1, at, part] = high - low


def node_modes(modes, slot, row):
    parts = parts_of(modes.shape[-1])
    found = [[] for _ in parts]
    for number in range(6):
        values = [modes[slot, number, row : row + TILE, part] for part in parts]
        for mine, value, after in zip(found, values, along_depth(values, 1)):
            mine.append(value + after)
            mine.append(after - value)
    return found


def element_energy(lower, upper, scale):
    def mode(component, first, second, third):
        index = 4 * component + 2 * second + third
        if first:
            return upper[index] - lower[index]
        return upper[index] + lower[index]

    def square(value):
        return value * value

    normal = [mode(0, 1, 0, 0), mode(1, 0, 1, 0), mode(2, 0, 0, 1)]
    trace = normal[0] + normal[1] + normal[2]
    main = square(mode(0, 0, 0, 1) + mode(2, 1, 0, 0))
    main = main + square(mode(1, 0, 0, 1) + mode(2, 0, 1, 0))
    main = main + square(mode(0, 0, 1, 0) + mode(1, 1, 0, 0))
    bent = [
        (mode(1, 0, 1, 1), mode(0, 1, 0, 1)),
        (mode(2, 0, 1, 1), mode(0, 1, 1, 0)),
        (mode(2, 1, 0, 1), mode(1, 1, 1, 0)),
    ]
    half = None
    for left, right in bent:
        main = main + square(left + right)
        term = square(left - right)
        half = term if half is None else half + term
    main = main + 2.0 * (square(normal[0]) + square(normal[1]) + square(normal[2]))
    main = main + 0.5 * half
    twisted = [mode(0, 0, 1, 1), mode(1, 1, 0, 1), mode(2, 1, 1, 0)]
    twists = square(twisted[0]) + square(twisted[1]) + square(twisted[2])
    twists = twists + square(twisted[0] + twisted[1] + twisted[2])
    warps = square(mode(0, 1, 1, 1)) + square(mode(1, 1, 1, 1)) + square(mode(2, 1, 1, 1))
    shear, bulk, twist, warp = scale
    return (shear * main + bulk * square(trace)) + (twist * twists + warp * warps)


def shares(ratio):
    total = ratio[0]
    for case in range(1, ratio.shape[0]):
        total = total + ratio[case]
    total = filled((TILE, LANES), total.astype(jnp.float32))

    def scale(case):
        share = filled((TILE, LANES), ratio[case].astype(jnp.float32)) / total
        return [factor * share for factor in energy_factors()]

    return scale


def flag(condition):
    return jnp.where(condition, 1.0, 0.0).astype(jnp.float32)


def y_flags():
    rank = lax.axis_index("gy")
    return flag(rank > 0), flag(rank < lax.axis_size("gy") - 1)


def free_of(mask):
    return (1 - mask).astype(jnp.float32)


def prepare_kernel(sides, displacement, fixed, density, void, *refs):
    count = len(sides)
    moved, design = refs[:2]
    packs = refs[2 : 2 + count]
    nodes, mask, node_edge, mask_edge, design_edge, void_edge, sems = refs[2 + count :]
    layers, rows, depth = density.shape
    core = lax.axis_index("lc")
    copies = [
        pltpu.make_async_copy(displacement.at[0, :, 0], nodes, sems.at[0]),
        pltpu.make_async_copy(fixed.at[0], mask, sems.at[1]),
        pltpu.make_async_copy(
            density.at[pl.ds(core * (layers - 2), 2)], design.at[:, pl.ds(0, rows)], sems.at[2]
        ),
    ]
    for number, side in enumerate(sides):
        if side == "both":
            start = pl.multiple_of((1 - lax.axis_index("gy")) * (rows - TILE), TILE)
        else:
            start = 0 if side == "first" else rows - TILE
        at = pl.ds(start, TILE)
        base = 3 + 4 * number
        copies += [
            pltpu.make_async_copy(displacement.at[0, :, :, at], node_edge.at[number], sems.at[base]),
            pltpu.make_async_copy(fixed.at[:, at], mask_edge.at[number], sems.at[base + 1]),
            pltpu.make_async_copy(density.at[:, at], design_edge.at[number], sems.at[base + 2]),
            pltpu.make_async_copy(void.at[:, at], void_edge.at[number], sems.at[base + 3]),
        ]
    for copy in copies:
        copy.start()
    for copy in copies:
        copy.wait()
    free = free_of(mask[...])
    front = lax.broadcasted_iota(jnp.int32, (TILE, depth), 0) < SLOT
    for component in range(3):
        value = nodes[component] * free
        moved[component, 0:rows, :] = value
        moved[component, rows : rows + TILE, :] = jnp.where(front, value[:TILE], value[rows - TILE :])
    for layer in range(2):
        first, last = design[layer, 0:TILE, :], design[layer, rows - TILE : rows, :]
        design[layer, rows : rows + TILE, :] = jnp.where(front, first, last)

    for number, (side, packed) in enumerate(zip(sides, packs)):
        if side == "both":
            from_last = lax.axis_index("gy") == 0
        else:
            from_last = side == "last"

        def edge(tile):
            if side == "first":
                return tile[0:SLOT]
            turned = pltpu.roll(tile, SLOT, 0)
            if side == "last":
                return turned[0:SLOT]
            return jnp.where(from_last, turned, tile)[0:SLOT]

        for layer in range(layers):
            free = free_of(mask_edge[number, layer])
            for component in range(3):
                packed[component * layers + layer] = edge(free * node_edge[number, component, layer])
            packed[3 * layers + layer] = edge(design_edge[number, layer])
            packed[4 * layers + layer] = edge(free_of(void_edge[number, layer]))


def pack_kernel(sides, moved, partner, design, crossing, *corners):
    rows = crossing.shape[1]
    for source, base in ((moved, 0), (partner, 3), (design, 6)):
        for index in range(source.shape[0]):
            crossing[base + index] = source[index, 0:rows, :]
            for side, corner in zip(sides, corners):
                first = source[index, rows : rows + SLOT, :]
                last = source[index, rows + SLOT : rows + TILE, :]
                if side == "both":
                    corner[base + index] = jnp.where(lax.axis_index("gy") == 0, last, first)
                else:
                    corner[base + index] = first if side == "first" else last


def energy_kernel(count, displacement, fixed, ratio, *refs):
    halos = refs[:count]
    mine, theirs, last, nodes, modes, energy = refs[count:]
    layers, rows, depth = fixed.shape
    wide = rows + TILE
    half = layers // 2
    core = lax.axis_index("lc")
    has_left, has_right = y_flags()
    for layer in range(layers):
        free = free_of(fixed[layer])
        for component in range(3):
            nodes[component, layer, 0:rows, :] = displacement[0, component, layer] * free
            at = component * layers + layer
            nodes[component, layer, rows : rows + SLOT, :] = halos[-1][at] * has_right
            nodes[component, layer, rows + SLOT : wide, :] = halos[0][at] * has_left
        row_modes(nodes, modes, layer, layer, wide)
    scale = shares(ratio)(core)
    for row in range(0, wide, TILE):
        lower = node_modes(modes, 0, row)
        for layer in range(layers - 1):
            upper = node_modes(modes, layer + 1, row)
            for part, below, above in zip(parts_of(depth), lower, upper):
                energy[layer, row : row + TILE, part] = element_energy(below, above, scale)
            lower = upper
    for component in range(3):
        last[component] = nodes[component, layers - 1]
    mine[0 : half - 1] = energy[pl.ds(core * half, half - 1)]

    @pl.when(core == 0)
    def _():
        mine[half - 1] = energy[half - 1]
        theirs[0 : half - 1] = energy[half : layers - 1]
        theirs[half : half + 3] = nodes[:, layers - 1]

    @pl.when(core == 1)
    def _():
        theirs[0:half] = energy[0:half]


def scaling_kernel(count, density, void, beyond, *refs):
    halos, corners = refs[:count], refs[count : 2 * count]
    scaling, design, sums, halo_alive = refs[2 * count :]
    layers, rows, depth = density.shape
    wide = rows + TILE
    half = layers // 2
    core = lax.axis_index("lc")
    has_left, has_right = y_flags()
    start = core * half

    def place(slot, middle, left, right):
        design[slot, 0:rows, :] = middle
        design[slot, rows : rows + SLOT, :] = right * has_right
        design[slot, rows + SLOT : wide, :] = left * has_left

    for index in range(half + 2):
        source = index + core * (half - 2)
        at = 3 * layers + source
        place(index + 2 * (1 - core), density[source], halos[0][at], halos[-1][at])
    for index in range(2):
        place(core * (half + 2) + index, beyond[6 + index], corners[0][6 + index], corners[-1][6 + index])
    for layer in range(half):
        at = 4 * layers + start + layer
        halo_alive[layer, 0:SLOT, :] = halos[-1][at] * has_right
        halo_alive[layer, SLOT:TILE, :] = halos[0][at] * has_left
    row_sums(design, sums, range(half + 4), wide)

    total_x = layers * lax.axis_size("gz")
    total_y = rows * lax.axis_size("gy")
    first_layer = lax.axis_index("gz") * layers + start
    first_row = lax.axis_index("gy") * rows
    parts = parts_of(depth)
    lane = lane_index()

    def depth_count(number, distance):
        held = filled((TILE, LANES), 2.0)
        if number == 0:
            held = jnp.where(lane < distance, 1.0, held)
        if number == len(parts) - 1:
            held = jnp.where(lane >= LANES - distance, held - 1.0, held)
        return held

    counts = [(depth_count(number, 1), depth_count(number, 2)) for number in range(len(parts))]

    def inside(at):
        return flag((at >= 0) & (at < total_x))

    for row in range(0, wide, TILE):
        column = row_index() + (first_row + row)
        if row == rows:
            column = jnp.where(row_index() >= SLOT, column - (rows + TILE), column)

        def within(offset):
            at = column + offset
            return jnp.where((at >= 0) & (at < total_y), 1.0, 0.0)

        y0, y1, y2 = within(0), within(-1) + within(1), within(-2) + within(2)
        for layer in range(half):
            filtered = cone_tile(design, sums, layer + 2, row)
            at = first_layer + layer
            x1 = inside(at - 1) + inside(at + 1)
            x2 = inside(at - 2) + inside(at + 2)
            level0, level1, level2 = depth_levels(
                y0, x1 * y0 + y1, x1 * y1, x2 * y0 + y2, x1 * y2 + x2 * y1
            )
            for part, value, (count1, count2) in zip(parts, filtered, counts):
                weight_sum = jnp.maximum(level0 + count1 * level1 + count2 * level2, 1.0)
                inverse = 1.0 / weight_sum
                physical = value * inverse
                value = (-3.0 * (1.0 - 0.001)) * physical * physical * inverse
                if row == rows:
                    alive = halo_alive[layer, :, part]
                else:
                    alive = free_of(void[start + layer, row : row + TILE, part])
                scaling[layer, row : row + TILE, part] = value * alive


def sensed_kernel(count, scaling, mine, received, last, ratio, above, *refs):
    corners = refs[:count]
    sensed, outgoing, nodes, modes = refs[count:]
    half, wide, depth = scaling.shape
    rows = wide - TILE
    core = lax.axis_index("lc")
    for layer in range(half - 1):
        sensed[layer] = scaling[layer] * (mine[layer] + received[layer])

    @pl.when(core == 0)
    def _():
        sensed[half - 1] = scaling[half - 1] * (mine[half - 1] + received[half - 1])
        outgoing[...] = sensed[0:2]

    @pl.when(core == 1)
    def _():
        has_left, has_right = y_flags()
        scales = shares(ratio)
        for case in range(2):
            for component in range(3):
                at = 3 * case + component
                if case == 0:
                    nodes[component, 2 * case] = received[half + component]
                else:
                    nodes[component, 2 * case] = last[component]
                nodes[component, 2 * case + 1, 0:rows, :] = above[at]
                nodes[component, 2 * case + 1, rows : rows + SLOT, :] = corners[-1][at] * has_right
                nodes[component, 2 * case + 1, rows + SLOT : wide, :] = corners[0][at] * has_left
            for index in (2 * case, 2 * case + 1):
                row_modes(nodes, modes, index, index, wide)
        for row in range(0, wide, TILE):
            totals = None
            for case in range(2):
                lower, upper = (node_modes(modes, 2 * case + side, row) for side in (0, 1))
                energies = [element_energy(a, b, scales(case)) for a, b in zip(lower, upper)]
                totals = energies if totals is None else [a + b for a, b in zip(totals, energies)]
            for part, value in zip(parts_of(depth), totals):
                sensed[half - 1, row : row + TILE, part] = scaling[half - 1, row : row + TILE, part] * value
        outgoing[...] = sensed[half - 2 : half]


def inner_kernel(void, own, other, gradient, field, sums):
    layers, rows, depth = void.shape
    wide = rows + TILE
    half = layers // 2
    core = lax.axis_index("lc")
    field[pl.ds(core * half, half)] = own[...]
    field[pl.ds((1 - core) * half, half)] = other[...]
    row_sums(field, sums, range(layers), wide)
    for row in range(0, rows, TILE):
        for layer in range(2, layers - 2):
            filtered = cone_tile(field, sums, layer, row)
            for part, value in zip(parts_of(depth), filtered):
                alive = free_of(void[layer, row : row + TILE, part])
                gradient[layer - 2, row : row + TILE, part] = alive * value


def side_rows(side, void, own, beyond, result, field, sums):
    layers, rows, depth = void.shape
    half = own.shape[0]
    field[pl.ds(side * 4, 2)] = beyond[...]
    field[pl.ds(2 - 2 * side, 4)] = own[pl.ds(side * (half - 4), 4)]
    row_sums(field, sums, range(6), rows + TILE)
    base = side * (layers - 2)
    for row in range(0, rows, TILE):
        for layer in range(2):
            filtered = cone_tile(field, sums, layer + 2, row)
            for part, value in zip(parts_of(depth), filtered):
                alive = free_of(void[base + layer, row : row + TILE, part])
                result[layer, row : row + TILE, part] = alive * value


def near_kernel(void, own, beyond, result, field, sums):
    side_rows(lax.axis_index("lc"), void, own, beyond, result, field, sums)


def far_kernel(void, other, beyond, inner, near, gradient, field, sums, far, sems):
    layers = void.shape[0]
    core = lax.axis_index("lc")
    copies = [
        pltpu.make_async_copy(inner, gradient.at[pl.ds(2, layers - 4)], sems.at[0]),
        pltpu.make_async_copy(near, gradient.at[pl.ds(core * (layers - 2), 2)], sems.at[1]),
        pltpu.make_async_copy(far, gradient.at[pl.ds((1 - core) * (layers - 2), 2)], sems.at[2]),
    ]
    for copy in copies[:2]:
        copy.start()
    side_rows(1 - core, void, other, beyond, far, field, sums)
    copies[2].start()
    for copy in copies:
        copy.wait()


def vmem():
    return pl.BlockSpec(memory_space=pltpu.VMEM)


def hbm():
    return pl.BlockSpec(memory_space=pltpu.HBM)


def call(kernel, outs, scratch, in_specs, flops, out_specs=None, sems=0, limit=24 << 20):
    scratch = [pltpu.VMEM(shape, kind) for shape, kind in scratch]
    if sems:
        scratch.append(pltpu.SemaphoreType.DMA((sems,)))
    return pl.pallas_call(
        kernel,
        out_shape=[jax.ShapeDtypeStruct(shape, jnp.float32) for shape in outs],
        in_specs=in_specs,
        out_specs=out_specs or [vmem()] * len(outs),
        scratch_shapes=scratch,
        cost_estimate=pl.CostEstimate(flops=flops, bytes_accessed=1 << 20, transcendentals=0),
        compiler_params=pltpu.CompilerParams(vmem_limit_bytes=limit),
    )


def shards(density, void_mask, fixed_mask, displacement, load_ratio):
    layers, rows, depth = density.shape
    half = layers // 2
    wide = rows + TILE
    gz, gy, lc = (lax.axis_size(axis) for axis in ("gz", "gy", "lc"))
    real = jnp.float32
    smem = pl.BlockSpec(memory_space=pltpu.SMEM)
    swap = [(0, 1), (1, 0)]
    crossing = []
    for z in range(1, gz):
        crossing.append((z * lc, (z - 1) * lc + 1))
        crossing.append(((z - 1) * lc + 1, z * lc))

    def y_pairs(step):
        if gy == 2:
            return [(y, 1 - y) for y in range(gy)]
        return [(y, y + step) for y in range(gy) if 0 <= y + step < gy]

    def diagonal(pairs, step):
        return [
            ((a // lc * gy + y) * lc + a % lc, (b // lc * gy + peer) * lc + b % lc)
            for a, b in pairs
            for y, peer in y_pairs(step)
        ]

    sides, steps = (["both"], [1]) if gy == 2 else (["first", "last"], [-1, 1])
    count = len(sides)

    kinds = [
        ((3, rows, depth), real),
        ((rows, depth), jnp.int32),
        ((count, 3, layers, TILE, depth), real),
        ((count, layers, TILE, depth), jnp.int32),
        ((count, layers, TILE, depth), real),
        ((count, layers, TILE, depth), jnp.int32),
    ]
    moved, design, *packs = call(
        functools.partial(prepare_kernel, sides),
        [(3, wide, depth), (2, wide, depth)] + [(5 * layers, SLOT, depth)] * count,
        kinds,
        [hbm()] * 4,
        1 << 18,
        sems=3 + 4 * count,
        limit=PREPARE_LIMIT,
    )(displacement, fixed_mask, density, void_mask)
    partner = lax.ppermute(moved, "lc", [(1, 0)])
    halos = [lax.ppermute(a, "gy", y_pairs(step)) for a, step in zip(packs, steps)][::-1]
    crossing_out, *corners = call(
        functools.partial(pack_kernel, sides),
        [(8, rows, depth)] + [(8, SLOT, depth)] * count,
        [],
        [vmem()] * 3,
        1 << 18,
    )(moved, partner, design)
    crossed = lax.ppermute(crossing_out, ("gz", "lc"), crossing)
    crossed_corners = [
        lax.ppermute(a, ("gz", "gy", "lc"), diagonal(crossing, step))
        for a, step in zip(corners, steps)
    ][::-1]

    mine, theirs, last = call(
        functools.partial(energy_kernel, count),
        [(half, wide, depth), (half + 3, wide, depth), (3, wide, depth)],
        [((3, layers, wide, depth), real), ((layers, 6, wide, depth), real), ((layers, wide, depth), real)],
        [vmem(), vmem(), smem] + [vmem()] * count,
        1 << 24,
    )(displacement, fixed_mask, load_ratio, *halos)
    received = lax.ppermute(theirs, "lc", swap)
    (scaling,) = call(
        functools.partial(scaling_kernel, count),
        [(half, wide, depth)],
        [((half + 4, wide, depth), real), ((half + 4, 2, wide, depth), real), ((half, TILE, depth), real)],
        [vmem()] * (3 + 2 * count),
        1 << 22,
    )(density, void_mask, crossed, *halos, *crossed_corners)
    sensed, outgoing = call(
        functools.partial(sensed_kernel, count),
        [(half, wide, depth), (2, wide, depth)],
        [((3, 4, wide, depth), real), ((4, 6, wide, depth), real)],
        [vmem()] * 4 + [smem] + [vmem()] * (1 + count),
        1 << 22,
    )(scaling, mine, received, last, load_ratio, crossed, *crossed_corners)
    own_beyond = lax.ppermute(outgoing, ("gz", "lc"), crossing)
    other = lax.ppermute(sensed, "lc", swap)
    (inner,) = call(
        inner_kernel,
        [(layers - 4, rows, depth)],
        [((layers, wide, depth), real), ((layers, 2, wide, depth), real)],
        [vmem()] * 3,
        1 << 22,
    )(void_mask, sensed, other)
    other_beyond = lax.ppermute(own_beyond, "lc", swap)
    ends = [((6, wide, depth), real), ((6, 2, wide, depth), real)]
    (near,) = call(near_kernel, [(2, rows, depth)], ends, [vmem()] * 3, 1 << 21)(
        void_mask, sensed, own_beyond
    )
    (gradient,) = call(
        far_kernel,
        [(layers, rows, depth)],
        ends + [((2, rows, depth), real)],
        [vmem()] * 5,
        1 << 21,
        out_specs=[hbm()],
        sems=3,
    )(void_mask, other, other_beyond, inner, near)
    return gradient


def solution(mesh):
    placed = (
        P(("parts", "gz"), "gy", None),
        P(("parts", "gz"), "gy", None),
        P(("parts", "gz"), "gy", None),
        P("lc", None, ("parts", "gz"), "gy", None),
        P("parts"),
    )
    return jax.shard_map(
        shards,
        mesh=mesh,
        in_specs=placed,
        out_specs=P(("parts", "gz"), "gy", None),
        check_vma=False,
    )
```

```python
import functools
import math

import jax
import jax.numpy as jnp
from jax import lax
from jax.experimental import pallas as pl
from jax.experimental.pallas import tpu as pltpu
from jax.sharding import PartitionSpec as P

TILE = 8
SLOT = 4
LANES = 128
PREPARE_LIMIT = 53 << 20
WEIGHT = [2.5 - math.sqrt(squared) for squared in range(7)]


def energy_factors():
    poisson = 0.3
    factor = 1.0 / ((1.0 + poisson) * (1.0 - 2.0 * poisson))
    shear = factor * (0.5 - poisson) / 16.0
    bulk = factor * poisson / 16.0
    twist = factor * (0.5 - poisson) / 48.0
    warp = factor * ((1.0 - poisson) + 2.0 * (0.5 - poisson)) / 144.0
    return shear, bulk, twist, warp


def filled(shape, value=0.0):
    return jnp.full(shape, value, jnp.float32)


def lane_index():
    return lax.broadcasted_iota(jnp.int32, (TILE, LANES), 1)


def row_index():
    return lax.broadcasted_iota(jnp.int32, (TILE, LANES), 0)


def parts_of(depth):
    return [slice(at, at + LANES) for at in range(0, depth, LANES)]


def along_depth(values, offset):
    lane = lane_index()
    turned = [pltpu.roll(value, (-offset) % LANES, 1) for value in values]
    zero = filled((TILE, LANES))
    if offset > 0:
        keep, beyond = lane < LANES - offset, turned[1:] + [zero]
    else:
        keep, beyond = lane >= -offset, [zero] + turned[:-1]
    return [jnp.where(keep, own, other) for own, other in zip(turned, beyond)]


def along_rows(tiles, offset):
    turned = [pltpu.roll(tile, (-offset) % TILE, 0) for tile in tiles]
    if offset > 0:
        keep, beyond = row_index() < TILE - offset, turned[1:] + turned[:1]
    else:
        keep, beyond = row_index() >= -offset, turned[-1:] + turned[:-1]
    return [jnp.where(keep, own, other) for own, other in zip(turned, beyond)]


def row_sums(source, sums, layers, wide):
    depth = source.shape[-1]
    for layer in layers:
        for part in parts_of(depth):
            tiles = [source[layer, row : row + TILE, part] for row in range(0, wide, TILE)]
            for number, distance in enumerate((1, 2)):
                ahead, behind = along_rows(tiles, distance), along_rows(tiles, -distance)
                for index, (one, other) in enumerate(zip(ahead, behind)):
                    sums[layer, number, TILE * index : TILE * (index + 1), part] = one + other


def depth_levels(plain, near, corner, far, knight):
    w = WEIGHT
    level0 = w[0] * plain + w[1] * near + w[2] * corner + w[4] * far + w[5] * knight
    level1 = w[1] * plain + w[2] * near + w[3] * corner + w[5] * far + w[6] * knight
    level2 = w[4] * plain + w[5] * near + w[6] * corner
    return level0, level1, level2


def cone_tile(source, sums, layer, row):
    results = []
    for part in parts_of(source.shape[-1]):

        def plane(at):
            return source[layer + at, row : row + TILE, part]

        def summed(at, number):
            return sums[layer + at, number, row : row + TILE, part]

        near = (plane(-1) + plane(1)) + summed(0, 0)
        corner = summed(-1, 0) + summed(1, 0)
        far = (plane(-2) + plane(2)) + summed(0, 1)
        knight = (summed(-1, 1) + summed(1, 1)) + (summed(-2, 0) + summed(2, 0))
        results.append(depth_levels(plane(0), near, corner, far, knight))
    level1 = [levels[1] for levels in results]
    level2 = [levels[2] for levels in results]
    shifted = [along_depth(level1, 1), along_depth(level1, -1), along_depth(level2, 2), along_depth(level2, -2)]
    return [
        levels[0] + ((one + two) + (three + four))
        for levels, one, two, three, four in zip(results, *shifted)
    ]


def row_modes(nodes, modes, layer, slot, wide):
    for component in range(3):
        for part in parts_of(nodes.shape[-1]):
            tiles = [nodes[component, layer, row : row + TILE, part] for row in range(0, wide, TILE)]
            for index, (low, high) in enumerate(zip(tiles, along_rows(tiles, 1))):
                at = slice(TILE * index, TILE * (index + 1))
                modes[slot, 2 * component, at, part] = low + high
                modes[slot, 2 * component + 1, at, part] = high - low


def node_modes(modes, slot, row):
    parts = parts_of(modes.shape[-1])
    found = [[] for _ in parts]
    for number in range(6):
        values = [modes[slot, number, row : row + TILE, part] for part in parts]
        for mine, value, after in zip(found, values, along_depth(values, 1)):
            mine.append(value + after)
            mine.append(after - value)
    return found


def element_energy(lower, upper, scale):
    def mode(component, first, second, third):
        index = 4 * component + 2 * second + third
        if first:
            return upper[index] - lower[index]
        return upper[index] + lower[index]

    def square(value):
        return value * value

    normal = [mode(0, 1, 0, 0), mode(1, 0, 1, 0), mode(2, 0, 0, 1)]
    trace = normal[0] + normal[1] + normal[2]
    main = square(mode(0, 0, 0, 1) + mode(2, 1, 0, 0))
    main = main + square(mode(1, 0, 0, 1) + mode(2, 0, 1, 0))
    main = main + square(mode(0, 0, 1, 0) + mode(1, 1, 0, 0))
    bent = [
        (mode(1, 0, 1, 1), mode(0, 1, 0, 1)),
        (mode(2, 0, 1, 1), mode(0, 1, 1, 0)),
        (mode(2, 1, 0, 1), mode(1, 1, 1, 0)),
    ]
    half = None
    for left, right in bent:
        main = main + square(left + right)
        term = square(left - right)
        half = term if half is None else half + term
    main = main + 2.0 * (square(normal[0]) + square(normal[1]) + square(normal[2]))
    main = main + 0.5 * half
    twisted = [mode(0, 0, 1, 1), mode(1, 1, 0, 1), mode(2, 1, 1, 0)]
    twists = square(twisted[0]) + square(twisted[1]) + square(twisted[2])
    twists = twists + square(twisted[0] + twisted[1] + twisted[2])
    warps = square(mode(0, 1, 1, 1)) + square(mode(1, 1, 1, 1)) + square(mode(2, 1, 1, 1))
    shear, bulk, twist, warp = scale
    return (shear * main + bulk * square(trace)) + (twist * twists + warp * warps)


def shares(ratio):
    total = ratio[0]
    for case in range(1, ratio.shape[0]):
        total = total + ratio[case]
    total = filled((TILE, LANES), total.astype(jnp.float32))

    def scale(case):
        share = filled((TILE, LANES), ratio[case].astype(jnp.float32)) / total
        return [factor * share for factor in energy_factors()]

    return scale


def flag(condition):
    return jnp.where(condition, 1.0, 0.0).astype(jnp.float32)


def y_flags():
    rank = lax.axis_index("gy")
    return flag(rank > 0), flag(rank < lax.axis_size("gy") - 1)


def beyond_flag():
    rank, core = lax.axis_index("gz"), lax.axis_index("lc")
    return flag((rank > 0) & (core == 0) | (rank < lax.axis_size("gz") - 1) & (core == 1))


def free_of(mask):
    return (1 - mask).astype(jnp.float32)


def edge_of(first, last, side):
    if side == "both":
        return jnp.where(lax.axis_index("gy") == 0, pltpu.roll(last, SLOT, 0), first)[0:SLOT]
    return first[0:SLOT] if side == "first" else pltpu.roll(last, SLOT, 0)[0:SLOT]


def prepare_kernel(sides, displacement, fixed, density, void, *refs):
    count = len(sides)
    crossing, corners, packs = refs[0], refs[1 : 1 + count], refs[1 + count : 1 + 2 * count]
    nodes, mask, node_edge, mask_edge, design_edge, void_edge, sems = refs[1 + 2 * count :]
    layers, rows, _ = density.shape
    core = lax.axis_index("lc")
    layer_out = core * (layers - 1)
    copies = [
        pltpu.make_async_copy(displacement.at[0, :, layer_out], nodes, sems.at[0]),
        pltpu.make_async_copy(fixed.at[layer_out], mask, sems.at[1]),
        pltpu.make_async_copy(
            density.at[pl.ds(core * (layers - 2), 2)], crossing.at[pl.ds(3, 2)], sems.at[2]
        ),
    ]
    for number, side in enumerate(sides):
        if side == "both":
            start = pl.multiple_of((1 - lax.axis_index("gy")) * (rows - TILE), TILE)
        else:
            start = 0 if side == "first" else rows - TILE
        at = pl.ds(start, TILE)
        base = 3 + 4 * number
        copies += [
            pltpu.make_async_copy(displacement.at[0, :, :, at], node_edge.at[number], sems.at[base]),
            pltpu.make_async_copy(fixed.at[:, at], mask_edge.at[number], sems.at[base + 1]),
            pltpu.make_async_copy(density.at[:, at], design_edge.at[number], sems.at[base + 2]),
            pltpu.make_async_copy(void.at[:, at], void_edge.at[number], sems.at[base + 3]),
        ]
    for copy in copies:
        copy.start()
    for copy in copies:
        copy.wait()
    free = free_of(mask[...])
    for component in range(3):
        crossing[component] = nodes[component] * free
    for side, corner in zip(sides, corners):
        for index in range(5):
            corner[index] = edge_of(crossing[index, 0:TILE, :], crossing[index, rows - TILE : rows, :], side)
    for number, (side, packed) in enumerate(zip(sides, packs)):
        for layer in range(layers):
            free = free_of(mask_edge[number, layer])
            for component in range(3):
                moved = free * node_edge[number, component, layer]
                packed[component * layers + layer] = edge_of(moved, moved, side)
            design = design_edge[number, layer]
            packed[3 * layers + layer] = edge_of(design, design, side)
            alive = free_of(void_edge[number, layer])
            packed[4 * layers + layer] = edge_of(alive, alive, side)


def energy_kernel(count, displacement, fixed, ratio, *refs):
    halos = refs[:count]
    mine, theirs, nodes, modes, energy = refs[count:]
    layers, rows, depth = fixed.shape
    wide = rows + TILE
    half = layers // 2
    core = lax.axis_index("lc")
    has_left, has_right = y_flags()
    for layer in range(layers):
        free = free_of(fixed[layer])
        for component in range(3):
            nodes[component, layer, 0:rows, :] = displacement[0, component, layer] * free
            at = component * layers + layer
            nodes[component, layer, rows : rows + SLOT, :] = halos[-1][at] * has_right
            nodes[component, layer, rows + SLOT : wide, :] = halos[0][at] * has_left
        row_modes(nodes, modes, layer, layer, wide)
    scale = shares(ratio)(core)
    for row in range(0, wide, TILE):
        lower = node_modes(modes, 0, row)
        for layer in range(layers - 1):
            upper = node_modes(modes, layer + 1, row)
            for part, below, above in zip(parts_of(depth), lower, upper):
                energy[layer, row : row + TILE, part] = element_energy(below, above, scale)
            lower = upper
    mine[0 : half - 1] = energy[pl.ds(core * half, half - 1)]
    theirs[half : half + 3] = nodes[:, (1 - core) * (layers - 1)]

    @pl.when(core == 0)
    def _():
        mine[half - 1] = energy[half - 1]
        theirs[0 : half - 1] = energy[half : layers - 1]
        theirs[half - 1] = energy[half - 1]

    @pl.when(core == 1)
    def _():
        theirs[0:half] = energy[0:half]
        mine[half - 1] = filled((wide, depth))

    @pl.when((core == 1) & (lax.axis_index("gz") == lax.axis_size("gz") - 1))
    def _():
        zero = [filled((TILE, LANES))] * 12
        for row in range(0, wide, TILE):
            for part, below in zip(parts_of(depth), node_modes(modes, layers - 1, row)):
                mine[half - 1, row : row + TILE, part] = element_energy(below, zero, scale)


def scaling_kernel(count, density, void, beyond, *refs):
    halos, corners = refs[:count], refs[count : 2 * count]
    scaling, design, sums, halo_alive = refs[2 * count :]
    layers, rows, depth = density.shape
    wide = rows + TILE
    half = layers // 2
    core = lax.axis_index("lc")
    has_left, has_right = y_flags()
    start = core * half

    has_beyond = beyond_flag()

    def place(slot, middle, left, right, keep=1.0):
        design[slot, 0:rows, :] = middle * keep
        design[slot, rows : rows + SLOT, :] = right * (keep * has_right)
        design[slot, rows + SLOT : wide, :] = left * (keep * has_left)

    for index in range(half + 2):
        source = index + core * (half - 2)
        at = 3 * layers + source
        place(index + 2 * (1 - core), density[source], halos[0][at], halos[-1][at])
    for index in range(2):
        at = 3 + index
        place(core * (half + 2) + index, beyond[at], corners[0][at], corners[-1][at], has_beyond)
    for layer in range(half):
        at = 4 * layers + start + layer
        halo_alive[layer, 0:SLOT, :] = halos[-1][at] * has_right
        halo_alive[layer, SLOT:TILE, :] = halos[0][at] * has_left
    row_sums(design, sums, range(half + 4), wide)

    total_x = layers * lax.axis_size("gz")
    total_y = rows * lax.axis_size("gy")
    first_layer = lax.axis_index("gz") * layers + start
    first_row = lax.axis_index("gy") * rows
    parts = parts_of(depth)
    lane = lane_index()

    def depth_count(number, distance):
        held = filled((TILE, LANES), 2.0)
        if number == 0:
            held = jnp.where(lane < distance, 1.0, held)
        if number == len(parts) - 1:
            held = jnp.where(lane >= LANES - distance, held - 1.0, held)
        return held

    counts = [(depth_count(number, 1), depth_count(number, 2)) for number in range(len(parts))]

    def inside(at):
        return flag((at >= 0) & (at < total_x))

    for row in range(0, wide, TILE):
        column = row_index() + (first_row + row)
        if row == rows:
            column = jnp.where(row_index() >= SLOT, column - (rows + TILE), column)

        def within(offset):
            at = column + offset
            return jnp.where((at >= 0) & (at < total_y), 1.0, 0.0)

        y0, y1, y2 = within(0), within(-1) + within(1), within(-2) + within(2)
        for layer in range(half):
            filtered = cone_tile(design, sums, layer + 2, row)
            at = first_layer + layer
            x1 = inside(at - 1) + inside(at + 1)
            x2 = inside(at - 2) + inside(at + 2)
            level0, level1, level2 = depth_levels(
                y0, x1 * y0 + y1, x1 * y1, x2 * y0 + y2, x1 * y2 + x2 * y1
            )
            for part, value, (count1, count2) in zip(parts, filtered, counts):
                weight_sum = jnp.maximum(level0 + count1 * level1 + count2 * level2, 1.0)
                inverse = 1.0 / weight_sum
                physical = value * inverse
                value = (-3.0 * (1.0 - 0.001)) * physical * physical * inverse
                if row == rows:
                    alive = halo_alive[layer, :, part]
                else:
                    alive = free_of(void[start + layer, row : row + TILE, part])
                scaling[layer, row : row + TILE, part] = value * alive


def sensed_kernel(count, scaling, mine, received, ratio, crossed, *refs):
    corners = refs[:count]
    sensed, outgoing, nodes, modes = refs[count:]
    half, wide, depth = scaling.shape
    rows = wide - TILE
    core = lax.axis_index("lc")
    has_left, has_right = y_flags()
    has_beyond = beyond_flag()
    for component in range(3):
        nodes[component, core, 0:rows, :] = crossed[component] * has_beyond
        nodes[component, core, rows : rows + SLOT, :] = corners[-1][component] * (has_beyond * has_right)
        nodes[component, core, rows + SLOT : wide, :] = corners[0][component] * (has_beyond * has_left)
        nodes[component, 1 - core] = received[half + component]
    for index in range(2):
        row_modes(nodes, modes, index, index, wide)
    scale = shares(ratio)(1 - core)
    between = 2 - core
    for row in range(0, wide, TILE):
        lower, upper = (node_modes(modes, index, row) for index in (0, 1))
        for part, below, above in zip(parts_of(depth), lower, upper):
            outgoing[between, row : row + TILE, part] = element_energy(below, above, scale)
    for layer in range(half):
        sensed[layer] = scaling[layer] * (mine[layer] + received[layer])

    @pl.when(core == 0)
    def _():
        outgoing[0:2] = sensed[0:2]

    @pl.when(core == 1)
    def _():
        outgoing[0] = sensed[half - 2]
        outgoing[2] = scaling[half - 1]


def ends_kernel(scaling, mine, outgoing, received, ends):
    half = scaling.shape[0]
    core = lax.axis_index("lc")

    has_beyond = beyond_flag()

    @pl.when(core == 0)
    def _():
        ends[0] = has_beyond * received[0]
        ends[1] = has_beyond * (received[2] * (received[1] + outgoing[2]))
        ends[2] = received[0]

    @pl.when(core == 1)
    def _():
        ends[0] = scaling[half - 1] * ((outgoing[1] + mine[half - 1]) + has_beyond * received[2])
        ends[1] = has_beyond * received[0]
        ends[2] = has_beyond * received[1]


def inner_kernel(void, own, other, gradient, field, sums):
    layers, rows, depth = void.shape
    half = layers // 2
    core = lax.axis_index("lc")
    field[pl.ds(core * half, half)] = own[...]
    field[pl.ds((1 - core) * half, half)] = other[...]
    row_sums(field, sums, range(1, layers - 1), rows + TILE)
    for row in range(0, rows, TILE):
        for layer in range(3, layers - 3):
            filtered = cone_tile(field, sums, layer, row)
            for part, value in zip(parts_of(depth), filtered):
                alive = free_of(void[layer, row : row + TILE, part])
                gradient[layer - 3, row : row + TILE, part] = alive * value


def side_rows(side, void, own, other, ends, result, field, sums):
    layers, rows, depth = void.shape
    half = own.shape[0]

    @pl.when(side == 0)
    def _():
        field[0:2] = ends[0:2]
        field[2:6] = own[0:4]
        field[6] = own[4] if half > 4 else other[0]

    @pl.when(side == 1)
    def _():
        field[0] = own[half - 5] if half > 4 else other[half - 1]
        field[1:4] = own[half - 4 : half - 1]
        field[4:7] = ends[...]

    row_sums(field, sums, range(7), rows + TILE)
    base = side * (layers - 3)
    for row in range(0, rows, TILE):
        for layer in range(3):
            filtered = cone_tile(field, sums, layer + 2, row)
            for part, value in zip(parts_of(depth), filtered):
                alive = free_of(void[base + layer, row : row + TILE, part])
                result[layer, row : row + TILE, part] = alive * value


def near_kernel(void, own, other, ends, result, field, sums):
    side_rows(lax.axis_index("lc"), void, own, other, ends, result, field, sums)


def far_kernel(void, own, other, ends, inner, near, gradient, field, sums, far, sems):
    layers = void.shape[0]
    core = lax.axis_index("lc")
    copies = [
        pltpu.make_async_copy(inner, gradient.at[pl.ds(3, layers - 6)], sems.at[0]),
        pltpu.make_async_copy(near, gradient.at[pl.ds(core * (layers - 3), 3)], sems.at[1]),
        pltpu.make_async_copy(far, gradient.at[pl.ds((1 - core) * (layers - 3), 3)], sems.at[2]),
    ]
    for copy in copies[:2]:
        copy.start()
    side_rows(1 - core, void, other, own, ends, far, field, sums)
    copies[2].start()
    for copy in copies:
        copy.wait()


def vmem():
    return pl.BlockSpec(memory_space=pltpu.VMEM)


def hbm():
    return pl.BlockSpec(memory_space=pltpu.HBM)


def call(kernel, outs, scratch, in_specs, flops, out_specs=None, sems=0, limit=24 << 20):
    scratch = [pltpu.VMEM(shape, kind) for shape, kind in scratch]
    if sems:
        scratch.append(pltpu.SemaphoreType.DMA((sems,)))
    return pl.pallas_call(
        kernel,
        out_shape=[jax.ShapeDtypeStruct(shape, jnp.float32) for shape in outs],
        in_specs=in_specs,
        out_specs=out_specs or [vmem()] * len(outs),
        scratch_shapes=scratch,
        cost_estimate=pl.CostEstimate(flops=flops, bytes_accessed=1 << 20, transcendentals=0),
        compiler_params=pltpu.CompilerParams(vmem_limit_bytes=limit),
    )


def shards(density, void_mask, fixed_mask, displacement, load_ratio):
    layers, rows, depth = density.shape
    half = layers // 2
    wide = rows + TILE
    gz, gy, lc = (lax.axis_size(axis) for axis in ("gz", "gy", "lc"))
    real = jnp.float32
    smem = pl.BlockSpec(memory_space=pltpu.SMEM)
    swap = [(0, 1), (1, 0)]
    across = []
    for z in range(1, gz):
        across.append((z * lc, (z - 1) * lc + 1))
        across.append(((z - 1) * lc + 1, z * lc))

    def y_pairs(step):
        if gy == 2:
            return [(y, 1 - y) for y in range(gy)]
        return [(y, y + step) for y in range(gy) if 0 <= y + step < gy]

    outermost = [0, gz * lc - 1] if gy % 2 == 0 else []

    def at(place, y):
        return (place // lc * gy + y) * lc + place % lc

    axes = ("gz", "gy", "lc")
    swaps = [(at(place, y), at(place, y ^ 1)) for place in outermost for y in range(gy)]
    crossing = [(at(a, y), at(b, y)) for a, b in across for y in range(gy)] + swaps

    def diagonal(step):
        pairs = [(at(a, y), at(b, peer)) for a, b in across for y, peer in y_pairs(step)]
        return pairs + swaps if gy == 2 else pairs

    sides, steps = (["both"], [1]) if gy == 2 else (["first", "last"], [-1, 1])
    count = len(sides)

    kinds = [
        ((3, rows, depth), real),
        ((rows, depth), jnp.int32),
        ((count, 3, layers, TILE, depth), real),
        ((count, layers, TILE, depth), jnp.int32),
        ((count, layers, TILE, depth), real),
        ((count, layers, TILE, depth), jnp.int32),
    ]
    crossing_out, *edges = call(
        functools.partial(prepare_kernel, sides),
        [(5, rows, depth)] + [(5, SLOT, depth)] * count + [(5 * layers, SLOT, depth)] * count,
        kinds,
        [hbm()] * 4,
        1 << 18,
        sems=3 + 4 * count,
        limit=PREPARE_LIMIT,
    )(displacement, fixed_mask, density, void_mask)
    crossed = lax.ppermute(crossing_out, axes, crossing)
    corners = [lax.ppermute(a, axes, diagonal(step)) for a, step in zip(edges[:count], steps)][::-1]
    halos = [lax.ppermute(a, "gy", y_pairs(step)) for a, step in zip(edges[count:], steps)][::-1]

    mine, theirs = call(
        functools.partial(energy_kernel, count),
        [(half, wide, depth), (half + 3, wide, depth)],
        [((3, layers, wide, depth), real), ((layers, 6, wide, depth), real), ((layers, wide, depth), real)],
        [vmem(), vmem(), smem] + [vmem()] * count,
        1 << 24,
    )(displacement, fixed_mask, load_ratio, *halos)
    received = lax.ppermute(theirs, "lc", swap)
    (scaling,) = call(
        functools.partial(scaling_kernel, count),
        [(half, wide, depth)],
        [((half + 4, wide, depth), real), ((half + 4, 2, wide, depth), real), ((half, TILE, depth), real)],
        [vmem()] * (3 + 2 * count),
        1 << 22,
    )(density, void_mask, crossed, *halos, *corners)
    sensed, outgoing = call(
        functools.partial(sensed_kernel, count),
        [(half, wide, depth), (3, wide, depth)],
        [((3, 2, wide, depth), real), ((2, 6, wide, depth), real)],
        [vmem()] * 3 + [smem] + [vmem()] * (1 + count),
        1 << 22,
    )(scaling, mine, received, load_ratio, crossed, *corners)
    beyond = lax.ppermute(outgoing, axes, crossing)
    other = lax.ppermute(sensed, "lc", swap)
    (inner,) = call(
        inner_kernel,
        [(layers - 6, rows, depth)],
        [((layers, wide, depth), real), ((layers, 2, wide, depth), real)],
        [vmem()] * 3,
        1 << 22,
    )(void_mask, sensed, other)
    (own_ends,) = call(ends_kernel, [(3, wide, depth)], [], [vmem()] * 4, 1 << 18)(
        scaling, mine, outgoing, beyond
    )
    other_ends = lax.ppermute(own_ends, "lc", swap)
    held = [((7, wide, depth), real), ((7, 2, wide, depth), real)]
    (near,) = call(near_kernel, [(3, rows, depth)], held, [vmem()] * 4, 1 << 21)(
        void_mask, sensed, other, own_ends
    )
    (gradient,) = call(
        far_kernel,
        [(layers, rows, depth)],
        held + [((3, rows, depth), real)],
        [vmem()] * 6,
        1 << 21,
        out_specs=[hbm()],
        sems=3,
    )(void_mask, sensed, other, other_ends, inner, near)
    return gradient


def solution(mesh):
    placed = (
        P(("parts", "gz"), "gy", None),
        P(("parts", "gz"), "gy", None),
        P(("parts", "gz"), "gy", None),
        P("lc", None, ("parts", "gz"), "gy", None),
        P("parts"),
    )
    return jax.shard_map(
        shards,
        mesh=mesh,
        in_specs=placed,
        out_specs=P(("parts", "gz"), "gy", None),
        check_vma=False,
    )
```

```python
import functools
import math

import jax
import jax.numpy as jnp
from jax import lax
from jax.experimental import pallas as pl
from jax.experimental.pallas import tpu as pltpu
from jax.sharding import PartitionSpec as P

TILE = 8
SLOT = 4
LANES = 128
PREPARE_LIMIT = 53 << 20
WEIGHT = [2.5 - math.sqrt(squared) for squared in range(7)]


def energy_factors():
    poisson = 0.3
    factor = 1.0 / ((1.0 + poisson) * (1.0 - 2.0 * poisson))
    shear = factor * (0.5 - poisson) / 16.0
    bulk = factor * poisson / 16.0
    twist = factor * (0.5 - poisson) / 48.0
    warp = factor * ((1.0 - poisson) + 2.0 * (0.5 - poisson)) / 144.0
    return shear, bulk, twist, warp


def filled(shape, value=0.0):
    return jnp.full(shape, value, jnp.float32)


def lane_index():
    return lax.broadcasted_iota(jnp.int32, (TILE, LANES), 1)


def row_index():
    return lax.broadcasted_iota(jnp.int32, (TILE, LANES), 0)


def parts_of(depth):
    return [slice(at, at + LANES) for at in range(0, depth, LANES)]


def along_depth(values, offset):
    lane = lane_index()
    turned = [pltpu.roll(value, (-offset) % LANES, 1) for value in values]
    zero = filled((TILE, LANES))
    if offset > 0:
        keep, beyond = lane < LANES - offset, turned[1:] + [zero]
    else:
        keep, beyond = lane >= -offset, [zero] + turned[:-1]
    return [jnp.where(keep, own, other) for own, other in zip(turned, beyond)]


def along_rows(tiles, offset):
    turned = [pltpu.roll(tile, (-offset) % TILE, 0) for tile in tiles]
    if offset > 0:
        keep, beyond = row_index() < TILE - offset, turned[1:] + turned[:1]
    else:
        keep, beyond = row_index() >= -offset, turned[-1:] + turned[:-1]
    return [jnp.where(keep, own, other) for own, other in zip(turned, beyond)]


def row_sums(source, sums, layers, wide):
    depth = source.shape[-1]
    for layer in layers:
        for part in parts_of(depth):
            tiles = [source[layer, row : row + TILE, part] for row in range(0, wide, TILE)]
            for number, distance in enumerate((1, 2)):
                ahead, behind = along_rows(tiles, distance), along_rows(tiles, -distance)
                for index, (one, other) in enumerate(zip(ahead, behind)):
                    sums[layer, number, TILE * index : TILE * (index + 1), part] = one + other


def depth_levels(plain, near, corner, far, knight):
    w = WEIGHT
    level0 = w[0] * plain + w[1] * near + w[2] * corner + w[4] * far + w[5] * knight
    level1 = w[1] * plain + w[2] * near + w[3] * corner + w[5] * far + w[6] * knight
    level2 = w[4] * plain + w[5] * near + w[6] * corner
    return level0, level1, level2


def cone_tile(source, sums, layer, row):
    results = []
    for part in parts_of(source.shape[-1]):

        def plane(at):
            return source[layer + at, row : row + TILE, part]

        def summed(at, number):
            return sums[layer + at, number, row : row + TILE, part]

        near = (plane(-1) + plane(1)) + summed(0, 0)
        corner = summed(-1, 0) + summed(1, 0)
        far = (plane(-2) + plane(2)) + summed(0, 1)
        knight = (summed(-1, 1) + summed(1, 1)) + (summed(-2, 0) + summed(2, 0))
        results.append(depth_levels(plane(0), near, corner, far, knight))
    level1 = [levels[1] for levels in results]
    level2 = [levels[2] for levels in results]
    shifted = [along_depth(level1, 1), along_depth(level1, -1), along_depth(level2, 2), along_depth(level2, -2)]
    return [
        levels[0] + ((one + two) + (three + four))
        for levels, one, two, three, four in zip(results, *shifted)
    ]


def row_modes(nodes, modes, layer, slot, wide):
    for component in range(3):
        for part in parts_of(nodes.shape[-1]):
            tiles = [nodes[component, layer, row : row + TILE, part] for row in range(0, wide, TILE)]
            for index, (low, high) in enumerate(zip(tiles, along_rows(tiles, 1))):
                at = slice(TILE * index, TILE * (index + 1))
                modes[slot, 2 * component, at, part] = low + high
                modes[slot, 2 * component + 1, at, part] = high - low


def node_modes(modes, slot, row):
    parts = parts_of(modes.shape[-1])
    found = [[] for _ in parts]
    for number in range(6):
        values = [modes[slot, number, row : row + TILE, part] for part in parts]
        for mine, value, after in zip(found, values, along_depth(values, 1)):
            mine.append(value + after)
            mine.append(after - value)
    return found


def element_energy(lower, upper, scale):
    def mode(component, first, second, third):
        index = 4 * component + 2 * second + third
        if first:
            return upper[index] - lower[index]
        return upper[index] + lower[index]

    def square(value):
        return value * value

    normal = [mode(0, 1, 0, 0), mode(1, 0, 1, 0), mode(2, 0, 0, 1)]
    trace = normal[0] + normal[1] + normal[2]
    main = square(mode(0, 0, 0, 1) + mode(2, 1, 0, 0))
    main = main + square(mode(1, 0, 0, 1) + mode(2, 0, 1, 0))
    main = main + square(mode(0, 0, 1, 0) + mode(1, 1, 0, 0))
    bent = [
        (mode(1, 0, 1, 1), mode(0, 1, 0, 1)),
        (mode(2, 0, 1, 1), mode(0, 1, 1, 0)),
        (mode(2, 1, 0, 1), mode(1, 1, 1, 0)),
    ]
    half = None
    for left, right in bent:
        main = main + square(left + right)
        term = square(left - right)
        half = term if half is None else half + term
    main = main + 2.0 * (square(normal[0]) + square(normal[1]) + square(normal[2]))
    main = main + 0.5 * half
    twisted = [mode(0, 0, 1, 1), mode(1, 1, 0, 1), mode(2, 1, 1, 0)]
    twists = square(twisted[0]) + square(twisted[1]) + square(twisted[2])
    twists = twists + square(twisted[0] + twisted[1] + twisted[2])
    warps = square(mode(0, 1, 1, 1)) + square(mode(1, 1, 1, 1)) + square(mode(2, 1, 1, 1))
    shear, bulk, twist, warp = scale
    return (shear * main + bulk * square(trace)) + (twist * twists + warp * warps)


def shares(ratio):
    values = [jnp.broadcast_to(ratio[case : case + 1, :], (TILE, LANES)) for case in range(ratio.shape[0])]
    values = [value.astype(jnp.float32) for value in values]
    total = values[0]
    for value in values[1:]:
        total = total + value

    def scale(case):
        chosen = values[0]
        for number, value in enumerate(values[1:], 1):
            chosen = jnp.where(case == number, value, chosen)
        share = chosen / total
        return [factor * share for factor in energy_factors()]

    return scale


def flag(condition):
    return jnp.where(condition, 1.0, 0.0).astype(jnp.float32)


def y_flags():
    rank = lax.axis_index("gy")
    return flag(rank > 0), flag(rank < lax.axis_size("gy") - 1)


def beyond_flag():
    rank, core = lax.axis_index("gz"), lax.axis_index("lc")
    return flag((rank > 0) & (core == 0) | (rank < lax.axis_size("gz") - 1) & (core == 1))


def free_of(mask):
    return (1 - mask).astype(jnp.float32)


def edge_of(first, last, side):
    if side == "both":
        return jnp.where(lax.axis_index("gy") == 0, pltpu.roll(last, SLOT, 0), first)[0:SLOT]
    return first[0:SLOT] if side == "first" else pltpu.roll(last, SLOT, 0)[0:SLOT]


def prepare_kernel(sides, displacement, fixed, density, void, *refs):
    count = len(sides)
    crossing, corners, firsts, rests = (refs[0], *(refs[1 + at * count : 1 + (at + 1) * count] for at in range(3)))
    nodes, mask, node_edge, mask_edge, design_edge, void_edge, sems = refs[1 + 3 * count :]
    layers, rows, _ = density.shape
    core = lax.axis_index("lc")
    layer_out = core * (layers - 1)
    copies = [
        pltpu.make_async_copy(displacement.at[0, :, layer_out], nodes, sems.at[0]),
        pltpu.make_async_copy(fixed.at[layer_out], mask, sems.at[1]),
        pltpu.make_async_copy(
            density.at[pl.ds(core * (layers - 2), 2)], crossing.at[pl.ds(3, 2)], sems.at[2]
        ),
    ]
    for number, side in enumerate(sides):
        if side == "both":
            start = pl.multiple_of((1 - lax.axis_index("gy")) * (rows - TILE), TILE)
        else:
            start = 0 if side == "first" else rows - TILE
        at = pl.ds(start, TILE)
        base = 3 + 4 * number
        copies += [
            pltpu.make_async_copy(displacement.at[0, :, :, at], node_edge.at[number], sems.at[base]),
            pltpu.make_async_copy(fixed.at[:, at], mask_edge.at[number], sems.at[base + 1]),
            pltpu.make_async_copy(density.at[:, at], design_edge.at[number], sems.at[base + 2]),
            pltpu.make_async_copy(void.at[:, at], void_edge.at[number], sems.at[base + 3]),
        ]
    for copy in copies:
        copy.start()
    for copy in copies:
        copy.wait()
    free = free_of(mask[...])
    for component in range(3):
        crossing[component] = nodes[component] * free
    for side, corner in zip(sides, corners):
        for index in range(5):
            corner[index] = edge_of(crossing[index, 0:TILE, :], crossing[index, rows - TILE : rows, :], side)
    early = first_layers(layers)
    for number, (side, first, rest) in enumerate(zip(sides, firsts, rests)):
        base = 3 * (layers - FIRST)
        for layer in range(layers):
            free = free_of(mask_edge[number, layer])
            for component in range(3):
                moved = free * node_edge[number, component, layer]
                if layer in early:
                    first[component * FIRST + early.index(layer)] = edge_of(moved, moved, side)
                else:
                    rest[component * (layers - FIRST) + layer - 3] = edge_of(moved, moved, side)
            design = design_edge[number, layer]
            rest[base + layer] = edge_of(design, design, side)
            alive = free_of(void_edge[number, layer])
            rest[base + layers + layer] = edge_of(alive, alive, side)


FIRST = 5


def first_layers(layers):
    return (0, 1, 2, layers - 2, layers - 1)


def node_halo(firsts, rests, component, layer, layers):
    early = first_layers(layers)
    if layer in early:
        at, packs = component * FIRST + early.index(layer), firsts
    else:
        at, packs = component * (layers - FIRST) + layer - 3, rests
    return packs[0][at], packs[-1][at]


def load_nodes(displacement, fixed, firsts, rests, layer, nodes, modes, slot):
    layers, rows, _ = fixed.shape
    wide = rows + TILE
    has_left, has_right = y_flags()
    free = free_of(fixed[layer])
    for component in range(3):
        nodes[component, slot, 0:rows, :] = displacement[0, component, layer] * free
        left, right = node_halo(firsts, rests, component, layer, layers)
        nodes[component, slot, rows : rows + SLOT, :] = right * has_right
        nodes[component, slot, rows + SLOT : wide, :] = left * has_left
    row_modes(nodes, modes, slot, slot, wide)


def first_energy(modes, energy, tiles, scale):
    depth = energy.shape[-1]
    for row in range(0, TILE * tiles, TILE):
        found = [node_modes(modes, slot, row) for slot in range(FIRST)]
        for index, slot in enumerate((0, 1, 3)):
            for part, below, above in zip(parts_of(depth), found[slot], found[slot + 1]):
                energy[index, row : row + TILE, part] = element_energy(below, above, scale)


def energy_bulk_kernel(displacement, fixed, ratio, energy, nodes, modes):
    layers, rows, _ = fixed.shape
    for slot, layer in enumerate(first_layers(layers)):
        free = free_of(fixed[layer])
        for component in range(3):
            nodes[component, slot] = displacement[0, component, layer] * free
        row_modes(nodes, modes, slot, slot, rows)
    scale = shares(ratio)(lax.axis_index("lc"))
    first_energy(modes, energy, rows // TILE - 1, scale)


def energy_first_kernel(count, displacement, fixed, ratio, bulk, *refs):
    halos = refs[:count]
    mine, theirs, nodes, modes, energy = refs[count:]
    layers, rows, _ = fixed.shape
    last = rows - TILE
    core = lax.axis_index("lc")
    has_left, has_right = y_flags()
    for slot, layer in enumerate(first_layers(layers)):
        free = free_of(fixed[layer, last:rows])
        free_next = free_of(fixed[layer, 0:TILE])
        for component in range(3):
            left, right = node_halo(halos, None, component, layer, layers)
            nodes[component, slot, 0:TILE, :] = displacement[0, component, layer, last:rows] * free
            nodes[component, slot, TILE : TILE + SLOT, :] = right * has_right
            nodes[component, slot, TILE + SLOT : 2 * TILE, :] = left * has_left
            nodes[component, slot, 2 * TILE : 3 * TILE, :] = displacement[0, component, layer, 0:TILE] * free_next
        row_modes(nodes, modes, slot, slot, 3 * TILE)
    first_energy(modes, energy, 2, shares(ratio)(core))

    def whole_layer(target, index, source):
        target[index, 0:last, :] = bulk[source]
        target[index, last : rows + TILE, :] = energy[source]

    def node_layer(layer, slot):
        free = free_of(fixed[layer])
        for component in range(3):
            theirs[2 + component, 0:rows, :] = displacement[0, component, layer] * free
            theirs[2 + component, rows : rows + TILE, :] = nodes[component, slot, TILE : 2 * TILE, :]

    @pl.when(core == 0)
    def _():
        whole_layer(mine, 0, 0)
        whole_layer(mine, 1, 1)
        whole_layer(theirs, 0, 2)
        whole_layer(theirs, 1, 2)
        node_layer(layers - 1, FIRST - 1)

    @pl.when(core == 1)
    def _():
        whole_layer(mine, 0, 2)
        whole_layer(mine, 1, 2)
        whole_layer(theirs, 0, 0)
        whole_layer(theirs, 1, 1)
        node_layer(0, 0)


def energy_rest_kernel(count, displacement, fixed, ratio, *refs):
    firsts, rests = refs[:count], refs[count : 2 * count]
    mine, theirs, nodes, modes, energy = refs[2 * count :]
    layers, rows, depth = fixed.shape
    wide = rows + TILE
    core = lax.axis_index("lc")
    for slot in range(layers - 3):
        load_nodes(displacement, fixed, firsts, rests, slot + 2, nodes, modes, slot)
    scale = shares(ratio)(core)
    for row in range(0, wide, TILE):
        lower = node_modes(modes, 0, row)
        for layer in range(layers - 4):
            upper = node_modes(modes, layer + 1, row)
            for part, below, above in zip(parts_of(depth), lower, upper):
                energy[layer, row : row + TILE, part] = element_energy(below, above, scale)
            lower = upper
    held = layers // 2 - 2
    mine[...] = energy[pl.ds(core * held, held)]
    theirs[...] = energy[pl.ds((1 - core) * held, held)]


def crown_kernel(count, displacement, fixed, ratio, *refs):
    firsts = refs[:count]
    crown, nodes, modes = refs[count:]
    layers, rows, depth = fixed.shape
    wide = rows + TILE
    core = lax.axis_index("lc")
    crown[0] = filled((wide, depth))

    @pl.when((core == 1) & (lax.axis_index("gz") == lax.axis_size("gz") - 1))
    def _():
        scale = shares(ratio)(core)
        load_nodes(displacement, fixed, firsts, None, layers - 1, nodes, modes, 0)
        zero = [filled((TILE, LANES))] * 12
        for row in range(0, wide, TILE):
            for part, below in zip(parts_of(depth), node_modes(modes, 0, row)):
                crown[0, row : row + TILE, part] = element_energy(below, zero, scale)


def place(design, slot, middle, left, right, keep=1.0):
    rows = middle.shape[0]
    has_left, has_right = y_flags()
    design[slot, 0:rows, :] = middle * keep
    design[slot, rows : rows + SLOT, :] = right * (keep * has_right)
    design[slot, rows + SLOT : rows + TILE, :] = left * (keep * has_left)


def scaling_first_kernel(count, density, void, beyond, *refs):
    halos, corners = refs[:count], refs[count : 2 * count]
    scaling, design, sums, halo_alive = refs[2 * count :]
    layers = density.shape[0]
    core = lax.axis_index("lc")
    has_beyond = beyond_flag()
    for index in range(4):
        source = index + core * (layers - 4)
        at = 3 * (layers - FIRST) + source
        place(design, index + 2 * (1 - core), density[source], halos[0][at], halos[-1][at])
    for index in range(2):
        at = 3 + index
        place(design, 4 * core + index, beyond[at], corners[0][at], corners[-1][at], has_beyond)
    scale_layers(core * (layers - 2), void, halos, scaling, design, sums, halo_alive)


def scaling_rest_kernel(count, density, void, *refs):
    halos = refs[:count]
    scaling, design, sums, halo_alive = refs[count:]
    layers = density.shape[0]
    half = layers // 2
    start = 2 + lax.axis_index("lc") * (half - 2)
    for index in range(half + 2):
        source = start - 2 + index
        at = 3 * (layers - FIRST) + source
        place(design, index, density[source], halos[0][at], halos[-1][at])
    scale_layers(start, void, halos, scaling, design, sums, halo_alive)


def scale_layers(start, void, halos, scaling, design, sums, halo_alive):
    layers, rows, depth = void.shape
    half = scaling.shape[0]
    wide = rows + TILE
    has_left, has_right = y_flags()
    for layer in range(half):
        at = 3 * (layers - FIRST) + layers + start + layer
        halo_alive[layer, 0:SLOT, :] = halos[-1][at] * has_right
        halo_alive[layer, SLOT:TILE, :] = halos[0][at] * has_left
    row_sums(design, sums, range(half + 4), wide)

    total_x = layers * lax.axis_size("gz")
    total_y = rows * lax.axis_size("gy")
    first_layer = lax.axis_index("gz") * layers + start
    first_row = lax.axis_index("gy") * rows
    parts = parts_of(depth)
    lane = lane_index()

    def depth_count(number, distance):
        held = filled((TILE, LANES), 2.0)
        if number == 0:
            held = jnp.where(lane < distance, 1.0, held)
        if number == len(parts) - 1:
            held = jnp.where(lane >= LANES - distance, held - 1.0, held)
        return held

    counts = [(depth_count(number, 1), depth_count(number, 2)) for number in range(len(parts))]

    def inside(at):
        return flag((at >= 0) & (at < total_x))

    for row in range(0, wide, TILE):
        column = row_index() + (first_row + row)
        if row == rows:
            column = jnp.where(row_index() >= SLOT, column - (rows + TILE), column)

        def within(offset):
            at = column + offset
            return jnp.where((at >= 0) & (at < total_y), 1.0, 0.0)

        y0, y1, y2 = within(0), within(-1) + within(1), within(-2) + within(2)
        for layer in range(half):
            filtered = cone_tile(design, sums, layer + 2, row)
            at = first_layer + layer
            x1 = inside(at - 1) + inside(at + 1)
            x2 = inside(at - 2) + inside(at + 2)
            level0, level1, level2 = depth_levels(
                y0, x1 * y0 + y1, x1 * y1, x2 * y0 + y2, x1 * y2 + x2 * y1
            )
            for part, value, (count1, count2) in zip(parts, filtered, counts):
                weight_sum = jnp.maximum(level0 + count1 * level1 + count2 * level2, 1.0)
                inverse = 1.0 / weight_sum
                physical = value * inverse
                value = (-3.0 * (1.0 - 0.001)) * physical * physical * inverse
                if row == rows:
                    alive = halo_alive[layer, :, part]
                else:
                    alive = free_of(void[start + layer, row : row + TILE, part])
                scaling[layer, row : row + TILE, part] = value * alive


def sensed_first_kernel(count, scaling, mine, received, ratio, crossed, *refs):
    corners = refs[:count]
    sensed, outgoing, nodes, modes = refs[count:]
    _, wide, depth = scaling.shape
    rows = wide - TILE
    core = lax.axis_index("lc")
    has_left, has_right = y_flags()
    has_beyond = beyond_flag()
    for component in range(3):
        nodes[component, core, 0:rows, :] = crossed[component] * has_beyond
        nodes[component, core, rows : rows + SLOT, :] = corners[-1][component] * (has_beyond * has_right)
        nodes[component, core, rows + SLOT : wide, :] = corners[0][component] * (has_beyond * has_left)
        nodes[component, 1 - core] = received[2 + component]
    for index in range(2):
        row_modes(nodes, modes, index, index, wide)
    scale = shares(ratio)(1 - core)
    between = 2 - core
    for row in range(0, wide, TILE):
        lower, upper = (node_modes(modes, index, row) for index in (0, 1))
        for part, below, above in zip(parts_of(depth), lower, upper):
            outgoing[between, row : row + TILE, part] = element_energy(below, above, scale)
    for layer in range(2):
        sensed[layer] = scaling[layer] * (mine[layer] + received[layer])

    @pl.when(core == 0)
    def _():
        outgoing[0:2] = sensed[0:2]

    @pl.when(core == 1)
    def _():
        outgoing[0] = sensed[0]
        outgoing[2] = scaling[1]


def sensed_rest_kernel(scaling, mine, received, first, sensed):
    core = lax.axis_index("lc")
    held = scaling.shape[0]
    sensed[pl.ds(core * held, 2)] = first[...]
    for layer in range(held):
        sensed[2 * (1 - core) + layer] = scaling[layer] * (mine[layer] + received[layer])


def ends_kernel(scaling, crown, outgoing, received, ends):
    core = lax.axis_index("lc")

    has_beyond = beyond_flag()

    @pl.when(core == 0)
    def _():
        ends[0] = has_beyond * received[0]
        ends[1] = has_beyond * (received[2] * (received[1] + outgoing[2]))
        ends[2] = received[0]

    @pl.when(core == 1)
    def _():
        ends[0] = scaling[1] * ((outgoing[1] + crown[0]) + has_beyond * received[2])
        ends[1] = has_beyond * received[0]
        ends[2] = has_beyond * received[1]


def inner_kernel(void, own, other, gradient, field, sums):
    layers, rows, depth = void.shape
    half = layers // 2
    core = lax.axis_index("lc")
    field[pl.ds(core * half, half)] = own[...]
    field[pl.ds((1 - core) * half, half)] = other[...]
    row_sums(field, sums, range(1, layers - 1), rows + TILE)
    for row in range(0, rows, TILE):
        for layer in range(3, layers - 3):
            filtered = cone_tile(field, sums, layer, row)
            for part, value in zip(parts_of(depth), filtered):
                alive = free_of(void[layer, row : row + TILE, part])
                gradient[layer - 3, row : row + TILE, part] = alive * value


def side_rows(side, void, own, other, ends, result, field, sums):
    layers, rows, depth = void.shape
    half = own.shape[0]

    @pl.when(side == 0)
    def _():
        field[0:2] = ends[0:2]
        field[2:6] = own[0:4]
        field[6] = own[4] if half > 4 else other[0]

    @pl.when(side == 1)
    def _():
        field[0] = own[half - 5] if half > 4 else other[half - 1]
        field[1:4] = own[half - 4 : half - 1]
        field[4:7] = ends[...]

    row_sums(field, sums, range(7), rows + TILE)
    base = side * (layers - 3)
    for row in range(0, rows, TILE):
        for layer in range(3):
            filtered = cone_tile(field, sums, layer + 2, row)
            for part, value in zip(parts_of(depth), filtered):
                alive = free_of(void[base + layer, row : row + TILE, part])
                result[layer, row : row + TILE, part] = alive * value


def near_kernel(void, own, other, ends, result, field, sums):
    side_rows(lax.axis_index("lc"), void, own, other, ends, result, field, sums)


def far_kernel(void, own, other, ends, inner, near, gradient, field, sums, far, sems):
    layers = void.shape[0]
    core = lax.axis_index("lc")
    copies = [
        pltpu.make_async_copy(inner, gradient.at[pl.ds(3, layers - 6)], sems.at[0]),
        pltpu.make_async_copy(near, gradient.at[pl.ds(core * (layers - 3), 3)], sems.at[1]),
        pltpu.make_async_copy(far, gradient.at[pl.ds((1 - core) * (layers - 3), 3)], sems.at[2]),
    ]
    for copy in copies[:2]:
        copy.start()
    side_rows(1 - core, void, other, own, ends, far, field, sums)
    copies[2].start()
    for copy in copies:
        copy.wait()


def vmem():
    return pl.BlockSpec(memory_space=pltpu.VMEM)


def hbm():
    return pl.BlockSpec(memory_space=pltpu.HBM)


def call(kernel, outs, scratch, in_specs, flops, out_specs=None, sems=0, limit=24 << 20):
    scratch = [pltpu.VMEM(shape, kind) for shape, kind in scratch]
    if sems:
        scratch.append(pltpu.SemaphoreType.DMA((sems,)))
    return pl.pallas_call(
        kernel,
        out_shape=[jax.ShapeDtypeStruct(shape, jnp.float32) for shape in outs],
        in_specs=in_specs,
        out_specs=out_specs or [vmem()] * len(outs),
        scratch_shapes=scratch,
        cost_estimate=pl.CostEstimate(flops=flops, bytes_accessed=1 << 20, transcendentals=0),
        compiler_params=pltpu.CompilerParams(vmem_limit_bytes=limit),
    )


def shards(density, void_mask, fixed_mask, displacement, load_ratio):
    layers, rows, depth = density.shape
    half = layers // 2
    wide = rows + TILE
    gz, gy, lc = (lax.axis_size(axis) for axis in ("gz", "gy", "lc"))
    real = jnp.float32
    load_ratio = load_ratio.reshape(-1, 1)
    swap = [(0, 1), (1, 0)]
    across = []
    for z in range(1, gz):
        across.append((z * lc, (z - 1) * lc + 1))
        across.append(((z - 1) * lc + 1, z * lc))

    def y_pairs(step):
        if gy == 2:
            return [(y, 1 - y) for y in range(gy)]
        return [(y, y + step) for y in range(gy) if 0 <= y + step < gy]

    parts = lax.axis_size("parts")
    axes = ("parts", "gz", "gy", "lc")

    def at(part, place, y):
        return ((part * gz + place // lc) * gy + y) * lc + place % lc

    swaps = []
    if parts % 2 == 0:
        for part in range(parts):
            for place in (0, gz * lc - 1):
                swaps += [(at(part, place, y), at(part ^ 1, place, y)) for y in range(gy)]

    def across_pairs(peers):
        return [
            (at(part, a, y), at(part, b, peer)) for part in range(parts) for a, b in across for y, peer in peers
        ]

    crossing = across_pairs([(y, y) for y in range(gy)]) + swaps

    def diagonal(step):
        pairs = across_pairs(y_pairs(step))
        return pairs + swaps if gy == 2 else pairs

    sides, steps = (["both"], [1]) if gy == 2 else (["first", "last"], [-1, 1])
    count = len(sides)

    kinds = [
        ((3, rows, depth), real),
        ((rows, depth), jnp.int32),
        ((count, 3, layers, TILE, depth), real),
        ((count, layers, TILE, depth), jnp.int32),
        ((count, layers, TILE, depth), real),
        ((count, layers, TILE, depth), jnp.int32),
    ]
    crossing_out, *edges = call(
        functools.partial(prepare_kernel, sides),
        [(5, rows, depth)]
        + [(size, SLOT, depth) for size in (5, 3 * FIRST, 5 * layers - 3 * FIRST) for _ in sides],
        kinds,
        [hbm()] * 4,
        1 << 18,
        sems=3 + 4 * count,
        limit=PREPARE_LIMIT,
    )(displacement, fixed_mask, density, void_mask)
    crossed = lax.ppermute(crossing_out, axes, crossing)
    corners = [lax.ppermute(a, axes, diagonal(step)) for a, step in zip(edges[:count], steps)][::-1]
    halos, rests = (
        [lax.ppermute(a, "gy", y_pairs(step)) for a, step in zip(packs, steps)][::-1]
        for packs in (edges[count : 2 * count], edges[2 * count :])
    )

    def energy(kernel, held, high, low, outs, *more):
        return call(
            kernel,
            outs,
            [((3, held, high, depth), real), ((held, 6, high, depth), real)] + low,
            [vmem()] * (3 + len(more)),
            1 << 23,
        )(displacement, fixed_mask, load_ratio, *more)

    def scaling(kernel, held, *more):
        (made,) = call(
            functools.partial(kernel, count),
            [(held, wide, depth)],
            [((held + 4, wide, depth), real), ((held + 4, 2, wide, depth), real), ((held, TILE, depth), real)],
            [vmem()] * (2 + len(more)),
            1 << 21,
        )(density, void_mask, *more)
        return made

    (bulk,) = energy(energy_bulk_kernel, FIRST, rows, [], [(3, rows - TILE, depth)])
    mine, theirs = energy(
        functools.partial(energy_first_kernel, count),
        FIRST,
        3 * TILE,
        [((3, 2 * TILE, depth), real)],
        [(2, wide, depth), (5, wide, depth)],
        bulk,
        *halos,
    )
    received = lax.ppermute(theirs, "lc", swap)
    scaling_rest = scaling(scaling_rest_kernel, half - 2, *rests)
    mine_rest, theirs_rest = energy(
        functools.partial(energy_rest_kernel, count),
        layers - 3,
        wide,
        [((layers - 4, wide, depth), real)],
        [(half - 2, wide, depth), (half - 2, wide, depth)],
        *halos,
        *rests,
    )
    (crown,) = energy(
        functools.partial(crown_kernel, count), 1, wide, [], [(1, wide, depth)], *halos
    )
    received_rest = lax.ppermute(theirs_rest, "lc", swap)
    scaling_first = scaling(scaling_first_kernel, 2, crossed, *rests, *corners)
    first, outgoing = call(
        functools.partial(sensed_first_kernel, count),
        [(2, wide, depth), (3, wide, depth)],
        [((3, 2, wide, depth), real), ((2, 6, wide, depth), real)],
        [vmem()] * (5 + count),
        1 << 22,
    )(scaling_first, mine, received, load_ratio, crossed, *corners)
    (sensed,) = call(sensed_rest_kernel, [(half, wide, depth)], [], [vmem()] * 4, 1 << 18)(
        scaling_rest, mine_rest, received_rest, first
    )
    beyond = lax.ppermute(outgoing, axes, crossing)
    other = lax.ppermute(sensed, "lc", swap)
    (inner,) = call(
        inner_kernel,
        [(layers - 6, rows, depth)],
        [((layers, wide, depth), real), ((layers, 2, wide, depth), real)],
        [vmem()] * 3,
        1 << 22,
    )(void_mask, sensed, other)
    (own_ends,) = call(ends_kernel, [(3, wide, depth)], [], [vmem()] * 4, 1 << 18)(
        scaling_first, crown, outgoing, beyond
    )
    other_ends = lax.ppermute(own_ends, "lc", swap)
    held = [((7, wide, depth), real), ((7, 2, wide, depth), real)]
    (near,) = call(near_kernel, [(3, rows, depth)], held, [vmem()] * 4, 1 << 21)(
        void_mask, sensed, other, own_ends
    )
    (gradient,) = call(
        far_kernel,
        [(layers, rows, depth)],
        held + [((3, rows, depth), real)],
        [vmem()] * 6,
        1 << 21,
        out_specs=[hbm()],
        sems=3,
    )(void_mask, sensed, other, other_ends, inner, near)
    return gradient


def solution(mesh):
    placed = (
        P(("parts", "gz"), "gy", None),
        P(("parts", "gz"), "gy", None),
        P(("parts", "gz"), "gy", None),
        P("lc", None, ("parts", "gz"), "gy", None),
        P("parts"),
    )
    return jax.shard_map(
        shards,
        mesh=mesh,
        in_specs=placed,
        out_specs=P(("parts", "gz"), "gy", None),
        check_vma=False,
    )
```

```python
import functools
import math

import jax
import jax.numpy as jnp
from jax import lax
from jax.experimental import pallas as pl
from jax.experimental.pallas import tpu as pltpu
from jax.sharding import PartitionSpec as P

TILE = 8
SLOT = 4
LANES = 128
PREPARE_LIMIT = 53 << 20
WEIGHT = [2.5 - math.sqrt(squared) for squared in range(7)]


def energy_factors():
    poisson = 0.3
    factor = 1.0 / ((1.0 + poisson) * (1.0 - 2.0 * poisson))
    shear = factor * (0.5 - poisson) / 16.0
    bulk = factor * poisson / 16.0
    twist = factor * (0.5 - poisson) / 48.0
    warp = factor * ((1.0 - poisson) + 2.0 * (0.5 - poisson)) / 144.0
    return shear, bulk, twist, warp


def filled(shape, value=0.0):
    return jnp.full(shape, value, jnp.float32)


def lane_index():
    return lax.broadcasted_iota(jnp.int32, (TILE, LANES), 1)


def row_index():
    return lax.broadcasted_iota(jnp.int32, (TILE, LANES), 0)


def parts_of(depth):
    return [slice(at, at + LANES) for at in range(0, depth, LANES)]


def along_depth(values, offset):
    lane = lane_index()
    turned = [pltpu.roll(value, (-offset) % LANES, 1) for value in values]
    zero = filled((TILE, LANES))
    if offset > 0:
        keep, beyond = lane < LANES - offset, turned[1:] + [zero]
    else:
        keep, beyond = lane >= -offset, [zero] + turned[:-1]
    return [jnp.where(keep, own, other) for own, other in zip(turned, beyond)]


def along_rows(tiles, offset):
    turned = [pltpu.roll(tile, (-offset) % TILE, 0) for tile in tiles]
    if offset > 0:
        keep, beyond = row_index() < TILE - offset, turned[1:] + turned[:1]
    else:
        keep, beyond = row_index() >= -offset, turned[-1:] + turned[:-1]
    return [jnp.where(keep, own, other) for own, other in zip(turned, beyond)]


def row_sums(source, sums, layers, wide):
    depth = source.shape[-1]
    for layer in layers:
        for part in parts_of(depth):
            tiles = [source[layer, row : row + TILE, part] for row in range(0, wide, TILE)]
            for number, distance in enumerate((1, 2)):
                ahead, behind = along_rows(tiles, distance), along_rows(tiles, -distance)
                for index, (one, other) in enumerate(zip(ahead, behind)):
                    sums[layer, number, TILE * index : TILE * (index + 1), part] = one + other


def depth_levels(plain, near, corner, far, knight):
    w = WEIGHT
    level0 = w[0] * plain + w[1] * near + w[2] * corner + w[4] * far + w[5] * knight
    level1 = w[1] * plain + w[2] * near + w[3] * corner + w[5] * far + w[6] * knight
    level2 = w[4] * plain + w[5] * near + w[6] * corner
    return level0, level1, level2


def cone_tile(source, sums, layer, row):
    results = []
    for part in parts_of(source.shape[-1]):

        def plane(at):
            return source[layer + at, row : row + TILE, part]

        def summed(at, number):
            return sums[layer + at, number, row : row + TILE, part]

        near = (plane(-1) + plane(1)) + summed(0, 0)
        corner = summed(-1, 0) + summed(1, 0)
        far = (plane(-2) + plane(2)) + summed(0, 1)
        knight = (summed(-1, 1) + summed(1, 1)) + (summed(-2, 0) + summed(2, 0))
        results.append(depth_levels(plane(0), near, corner, far, knight))
    level1 = [levels[1] for levels in results]
    level2 = [levels[2] for levels in results]
    shifted = [along_depth(level1, 1), along_depth(level1, -1), along_depth(level2, 2), along_depth(level2, -2)]
    return [
        levels[0] + ((one + two) + (three + four))
        for levels, one, two, three, four in zip(results, *shifted)
    ]


def row_modes(nodes, modes, layer, slot, wide):
    for component in range(3):
        for part in parts_of(nodes.shape[-1]):
            tiles = [nodes[component, layer, row : row + TILE, part] for row in range(0, wide, TILE)]
            for index, (low, high) in enumerate(zip(tiles, along_rows(tiles, 1))):
                at = slice(TILE * index, TILE * (index + 1))
                modes[slot, 2 * component, at, part] = low + high
                modes[slot, 2 * component + 1, at, part] = high - low


def node_modes(modes, slot, row):
    parts = parts_of(modes.shape[-1])
    found = [[] for _ in parts]
    for number in range(6):
        values = [modes[slot, number, row : row + TILE, part] for part in parts]
        for mine, value, after in zip(found, values, along_depth(values, 1)):
            mine.append(value + after)
            mine.append(after - value)
    return found


def element_energy(lower, upper, scale):
    def mode(component, first, second, third):
        index = 4 * component + 2 * second + third
        if first:
            return upper[index] - lower[index]
        return upper[index] + lower[index]

    def square(value):
        return value * value

    normal = [mode(0, 1, 0, 0), mode(1, 0, 1, 0), mode(2, 0, 0, 1)]
    trace = normal[0] + normal[1] + normal[2]
    main = square(mode(0, 0, 0, 1) + mode(2, 1, 0, 0))
    main = main + square(mode(1, 0, 0, 1) + mode(2, 0, 1, 0))
    main = main + square(mode(0, 0, 1, 0) + mode(1, 1, 0, 0))
    bent = [
        (mode(1, 0, 1, 1), mode(0, 1, 0, 1)),
        (mode(2, 0, 1, 1), mode(0, 1, 1, 0)),
        (mode(2, 1, 0, 1), mode(1, 1, 1, 0)),
    ]
    half = None
    for left, right in bent:
        main = main + square(left + right)
        term = square(left - right)
        half = term if half is None else half + term
    main = main + 2.0 * (square(normal[0]) + square(normal[1]) + square(normal[2]))
    main = main + 0.5 * half
    twisted = [mode(0, 0, 1, 1), mode(1, 1, 0, 1), mode(2, 1, 1, 0)]
    twists = square(twisted[0]) + square(twisted[1]) + square(twisted[2])
    twists = twists + square(twisted[0] + twisted[1] + twisted[2])
    warps = square(mode(0, 1, 1, 1)) + square(mode(1, 1, 1, 1)) + square(mode(2, 1, 1, 1))
    shear, bulk, twist, warp = scale
    return (shear * main + bulk * square(trace)) + (twist * twists + warp * warps)


def shares(ratio):
    values = [jnp.broadcast_to(ratio[case : case + 1, :], (TILE, LANES)) for case in range(ratio.shape[0])]
    values = [value.astype(jnp.float32) for value in values]
    total = values[0]
    for value in values[1:]:
        total = total + value

    def scale(case):
        chosen = values[0]
        for number, value in enumerate(values[1:], 1):
            chosen = jnp.where(case == number, value, chosen)
        share = chosen / total
        return [factor * share for factor in energy_factors()]

    return scale


def flag(condition):
    return jnp.where(condition, 1.0, 0.0).astype(jnp.float32)


def y_flags():
    rank = lax.axis_index("gy")
    return flag(rank > 0), flag(rank < lax.axis_size("gy") - 1)


def beyond_flag():
    rank, core = lax.axis_index("gz"), lax.axis_index("lc")
    return flag((rank > 0) & (core == 0) | (rank < lax.axis_size("gz") - 1) & (core == 1))


def free_of(mask):
    return (1 - mask).astype(jnp.float32)


def edge_of(first, last, side):
    if side == "both":
        return jnp.where(lax.axis_index("gy") == 0, pltpu.roll(last, SLOT, 0), first)[0:SLOT]
    return first[0:SLOT] if side == "first" else pltpu.roll(last, SLOT, 0)[0:SLOT]


def prepare_kernel(sides, displacement, fixed, density, void, *refs):
    count = len(sides)
    crossing, corners, firsts, rests = (refs[0], *(refs[1 + at * count : 1 + (at + 1) * count] for at in range(3)))
    nodes, mask, node_edge, mask_edge, design_edge, void_edge, sems = refs[1 + 3 * count :]
    layers, rows, _ = density.shape
    core = lax.axis_index("lc")
    layer_out = core * (layers - 1)
    copies = [
        pltpu.make_async_copy(displacement.at[0, :, layer_out], nodes, sems.at[0]),
        pltpu.make_async_copy(fixed.at[layer_out], mask, sems.at[1]),
        pltpu.make_async_copy(
            density.at[pl.ds(core * (layers - 2), 2)], crossing.at[pl.ds(3, 2)], sems.at[2]
        ),
    ]
    for number, side in enumerate(sides):
        if side == "both":
            start = pl.multiple_of((1 - lax.axis_index("gy")) * (rows - TILE), TILE)
        else:
            start = 0 if side == "first" else rows - TILE
        at = pl.ds(start, TILE)
        base = 3 + 4 * number
        copies += [
            pltpu.make_async_copy(displacement.at[0, :, :, at], node_edge.at[number], sems.at[base]),
            pltpu.make_async_copy(fixed.at[:, at], mask_edge.at[number], sems.at[base + 1]),
            pltpu.make_async_copy(density.at[:, at], design_edge.at[number], sems.at[base + 2]),
            pltpu.make_async_copy(void.at[:, at], void_edge.at[number], sems.at[base + 3]),
        ]
    for copy in copies:
        copy.start()
    for copy in copies:
        copy.wait()
    free = free_of(mask[...])
    for component in range(3):
        crossing[component] = nodes[component] * free
    for side, corner in zip(sides, corners):
        for index in range(5):
            corner[index] = edge_of(crossing[index, 0:TILE, :], crossing[index, rows - TILE : rows, :], side)
    early = first_layers(layers)
    for number, (side, first, rest) in enumerate(zip(sides, firsts, rests)):
        base = 3 * (layers - FIRST)
        for layer in range(layers):
            free = free_of(mask_edge[number, layer])
            for component in range(3):
                moved = free * node_edge[number, component, layer]
                if layer in early:
                    first[component * FIRST + early.index(layer)] = edge_of(moved, moved, side)
                else:
                    rest[component * (layers - FIRST) + layer - 3] = edge_of(moved, moved, side)
            design = design_edge[number, layer]
            rest[base + layer] = edge_of(design, design, side)
            alive = free_of(void_edge[number, layer])
            rest[base + layers + layer] = edge_of(alive, alive, side)


FIRST = 5


def first_layers(layers):
    return (0, 1, 2, layers - 2, layers - 1)


def node_halo(firsts, rests, component, layer, layers):
    early = first_layers(layers)
    if layer in early:
        at, packs = component * FIRST + early.index(layer), firsts
    else:
        at, packs = component * (layers - FIRST) + layer - 3, rests
    return packs[0][at], packs[-1][at]


def load_nodes(displacement, fixed, firsts, rests, layer, nodes, modes, slot):
    layers, rows, _ = fixed.shape
    wide = rows + TILE
    has_left, has_right = y_flags()
    free = free_of(fixed[layer])
    for component in range(3):
        nodes[component, slot, 0:rows, :] = displacement[0, component, layer] * free
        left, right = node_halo(firsts, rests, component, layer, layers)
        nodes[component, slot, rows : rows + SLOT, :] = right * has_right
        nodes[component, slot, rows + SLOT : wide, :] = left * has_left
    row_modes(nodes, modes, slot, slot, wide)


def first_energy(modes, energy, tiles, scale):
    depth = energy.shape[-1]
    for row in range(0, TILE * tiles, TILE):
        found = [node_modes(modes, slot, row) for slot in range(FIRST)]
        for index, slot in enumerate((0, 1, 3)):
            for part, below, above in zip(parts_of(depth), found[slot], found[slot + 1]):
                energy[index, row : row + TILE, part] = element_energy(below, above, scale)


def energy_bulk_kernel(displacement, fixed, ratio, energy, nodes, modes):
    layers, rows, _ = fixed.shape
    for slot, layer in enumerate(first_layers(layers)):
        free = free_of(fixed[layer])
        for component in range(3):
            nodes[component, slot] = displacement[0, component, layer] * free
        row_modes(nodes, modes, slot, slot, rows)
    scale = shares(ratio)(lax.axis_index("lc"))
    first_energy(modes, energy, rows // TILE - 1, scale)


def energy_first_kernel(count, displacement, fixed, ratio, bulk, *refs):
    halos = refs[:count]
    mine, theirs, nodes, modes, energy = refs[count:]
    layers, rows, _ = fixed.shape
    last = rows - TILE
    core = lax.axis_index("lc")
    has_left, has_right = y_flags()
    for slot, layer in enumerate(first_layers(layers)):
        free = free_of(fixed[layer, last:rows])
        free_next = free_of(fixed[layer, 0:TILE])
        for component in range(3):
            left, right = node_halo(halos, None, component, layer, layers)
            nodes[component, slot, 0:TILE, :] = displacement[0, component, layer, last:rows] * free
            nodes[component, slot, TILE : TILE + SLOT, :] = right * has_right
            nodes[component, slot, TILE + SLOT : 2 * TILE, :] = left * has_left
            nodes[component, slot, 2 * TILE : 3 * TILE, :] = displacement[0, component, layer, 0:TILE] * free_next
        row_modes(nodes, modes, slot, slot, 3 * TILE)
    first_energy(modes, energy, 2, shares(ratio)(core))

    def whole_layer(target, index, source):
        target[index, 0:last, :] = bulk[source]
        target[index, last : rows + TILE, :] = energy[source]

    def node_layer(layer, slot):
        free = free_of(fixed[layer])
        for component in range(3):
            theirs[2 + component, 0:rows, :] = displacement[0, component, layer] * free
            theirs[2 + component, rows : rows + TILE, :] = nodes[component, slot, TILE : 2 * TILE, :]

    @pl.when(core == 0)
    def _():
        whole_layer(mine, 0, 0)
        whole_layer(mine, 1, 1)
        whole_layer(theirs, 0, 2)
        whole_layer(theirs, 1, 2)
        node_layer(layers - 1, FIRST - 1)

    @pl.when(core == 1)
    def _():
        whole_layer(mine, 0, 2)
        whole_layer(mine, 1, 2)
        whole_layer(theirs, 0, 0)
        whole_layer(theirs, 1, 1)
        node_layer(0, 0)


def energy_rest_kernel(count, displacement, fixed, ratio, *refs):
    firsts, rests = refs[:count], refs[count : 2 * count]
    energy, nodes, modes = refs[2 * count :]
    layers, rows, depth = fixed.shape
    wide = rows + TILE
    core = lax.axis_index("lc")
    for slot in range(layers - 3):
        load_nodes(displacement, fixed, firsts, rests, slot + 2, nodes, modes, slot)
    scale = shares(ratio)(core)
    for row in range(0, wide, TILE):
        lower = node_modes(modes, 0, row)
        for layer in range(layers - 4):
            upper = node_modes(modes, layer + 1, row)
            for part, below, above in zip(parts_of(depth), lower, upper):
                energy[layer, row : row + TILE, part] = element_energy(below, above, scale)
            lower = upper


def crown_kernel(count, displacement, fixed, ratio, *refs):
    firsts = refs[:count]
    crown, nodes, modes = refs[count:]
    layers, rows, depth = fixed.shape
    wide = rows + TILE
    core = lax.axis_index("lc")
    crown[0] = filled((wide, depth))

    @pl.when((core == 1) & (lax.axis_index("gz") == lax.axis_size("gz") - 1))
    def _():
        scale = shares(ratio)(core)
        load_nodes(displacement, fixed, firsts, None, layers - 1, nodes, modes, 0)
        zero = [filled((TILE, LANES))] * 12
        for row in range(0, wide, TILE):
            for part, below in zip(parts_of(depth), node_modes(modes, 0, row)):
                crown[0, row : row + TILE, part] = element_energy(below, zero, scale)


def place(design, slot, middle, left, right, keep=1.0):
    rows = middle.shape[0]
    has_left, has_right = y_flags()
    design[slot, 0:rows, :] = middle * keep
    design[slot, rows : rows + SLOT, :] = right * (keep * has_right)
    design[slot, rows + SLOT : rows + TILE, :] = left * (keep * has_left)


def scaling_first_kernel(count, density, void, beyond, *refs):
    halos, corners = refs[:count], refs[count : 2 * count]
    scaling, design, sums, halo_alive = refs[2 * count :]
    layers = density.shape[0]
    core = lax.axis_index("lc")
    has_beyond = beyond_flag()
    for index in range(4):
        source = index + core * (layers - 4)
        at = 3 * (layers - FIRST) + source
        place(design, index + 2 * (1 - core), density[source], halos[0][at], halos[-1][at])
    for index in range(2):
        at = 3 + index
        place(design, 4 * core + index, beyond[at], corners[0][at], corners[-1][at], has_beyond)
    scale_layers(core * (layers - 2), void, halos, scaling, design, sums, halo_alive)


def scaling_rest_kernel(count, density, void, *refs):
    halos = refs[:count]
    scaling, design, sums, halo_alive = refs[count:]
    layers = density.shape[0]
    for layer in range(layers):
        at = 3 * (layers - FIRST) + layer
        place(design, layer, density[layer], halos[0][at], halos[-1][at])
    scale_layers(2, void, halos, scaling, design, sums, halo_alive)


def scale_layers(start, void, halos, scaling, design, sums, halo_alive):
    layers, rows, depth = void.shape
    half = scaling.shape[0]
    wide = rows + TILE
    has_left, has_right = y_flags()
    for layer in range(half):
        at = 3 * (layers - FIRST) + layers + start + layer
        halo_alive[layer, 0:SLOT, :] = halos[-1][at] * has_right
        halo_alive[layer, SLOT:TILE, :] = halos[0][at] * has_left
    row_sums(design, sums, range(half + 4), wide)

    total_x = layers * lax.axis_size("gz")
    total_y = rows * lax.axis_size("gy")
    first_layer = lax.axis_index("gz") * layers + start
    first_row = lax.axis_index("gy") * rows
    parts = parts_of(depth)
    lane = lane_index()

    def depth_count(number, distance):
        held = filled((TILE, LANES), 2.0)
        if number == 0:
            held = jnp.where(lane < distance, 1.0, held)
        if number == len(parts) - 1:
            held = jnp.where(lane >= LANES - distance, held - 1.0, held)
        return held

    counts = [(depth_count(number, 1), depth_count(number, 2)) for number in range(len(parts))]

    def inside(at):
        return flag((at >= 0) & (at < total_x))

    for row in range(0, wide, TILE):
        column = row_index() + (first_row + row)
        if row == rows:
            column = jnp.where(row_index() >= SLOT, column - (rows + TILE), column)

        def within(offset):
            at = column + offset
            return jnp.where((at >= 0) & (at < total_y), 1.0, 0.0)

        y0, y1, y2 = within(0), within(-1) + within(1), within(-2) + within(2)
        for layer in range(half):
            filtered = cone_tile(design, sums, layer + 2, row)
            at = first_layer + layer
            x1 = inside(at - 1) + inside(at + 1)
            x2 = inside(at - 2) + inside(at + 2)
            level0, level1, level2 = depth_levels(
                y0, x1 * y0 + y1, x1 * y1, x2 * y0 + y2, x1 * y2 + x2 * y1
            )
            for part, value, (count1, count2) in zip(parts, filtered, counts):
                weight_sum = jnp.maximum(level0 + count1 * level1 + count2 * level2, 1.0)
                inverse = 1.0 / weight_sum
                physical = value * inverse
                value = (-3.0 * (1.0 - 0.001)) * physical * physical * inverse
                if row == rows:
                    alive = halo_alive[layer, :, part]
                else:
                    alive = free_of(void[start + layer, row : row + TILE, part])
                scaling[layer, row : row + TILE, part] = value * alive


def sensed_first_kernel(count, scaling, mine, received, ratio, crossed, *refs):
    corners = refs[:count]
    sensed, outgoing, nodes, modes = refs[count:]
    _, wide, depth = scaling.shape
    rows = wide - TILE
    core = lax.axis_index("lc")
    has_left, has_right = y_flags()
    has_beyond = beyond_flag()
    for component in range(3):
        nodes[component, core, 0:rows, :] = crossed[component] * has_beyond
        nodes[component, core, rows : rows + SLOT, :] = corners[-1][component] * (has_beyond * has_right)
        nodes[component, core, rows + SLOT : wide, :] = corners[0][component] * (has_beyond * has_left)
        nodes[component, 1 - core] = received[2 + component]
    for index in range(2):
        row_modes(nodes, modes, index, index, wide)
    scale = shares(ratio)(1 - core)
    between = 2 - core
    for row in range(0, wide, TILE):
        lower, upper = (node_modes(modes, index, row) for index in (0, 1))
        for part, below, above in zip(parts_of(depth), lower, upper):
            outgoing[between, row : row + TILE, part] = element_energy(below, above, scale)
    for layer in range(2):
        sensed[layer] = scaling[layer] * (mine[layer] + received[layer])

    @pl.when(core == 0)
    def _():
        outgoing[0:2] = sensed[0:2]

    @pl.when(core == 1)
    def _():
        outgoing[0] = sensed[0]
        outgoing[2] = scaling[1]


def sensed_rest_kernel(scaling, mine, received, sensed):
    for layer in range(scaling.shape[0]):
        sensed[layer] = scaling[layer] * (mine[layer] + received[layer])


def ends_kernel(scaling, crown, outgoing, received, ends):
    core = lax.axis_index("lc")

    has_beyond = beyond_flag()

    @pl.when(core == 0)
    def _():
        ends[0] = has_beyond * received[0]
        ends[1] = has_beyond * (received[2] * (received[1] + outgoing[2]))
        ends[2] = received[0]

    @pl.when(core == 1)
    def _():
        ends[0] = scaling[1] * ((outgoing[1] + crown[0]) + has_beyond * received[2])
        ends[1] = has_beyond * received[0]
        ends[2] = has_beyond * received[1]


def inner_kernel(void, own, other, middle, gradient, field, sums):
    layers, rows, depth = void.shape
    core = lax.axis_index("lc")
    field[pl.ds(core * (layers - 2), 2)] = own[...]
    field[pl.ds((1 - core) * (layers - 2), 2)] = other[...]
    field[2 : layers - 2] = middle[...]
    row_sums(field, sums, range(1, layers - 1), rows + TILE)
    for row in range(0, rows, TILE):
        for layer in range(3, layers - 3):
            filtered = cone_tile(field, sums, layer, row)
            for part, value in zip(parts_of(depth), filtered):
                alive = free_of(void[layer, row : row + TILE, part])
                gradient[layer - 3, row : row + TILE, part] = alive * value


def side_rows(side, void, first, middle, ends, result, field, sums):
    layers, rows, depth = void.shape
    held = middle.shape[0]

    @pl.when(side == 0)
    def _():
        field[0:2] = ends[0:2]
        field[2:4] = first[...]
        field[4:7] = middle[0:3]

    @pl.when(side == 1)
    def _():
        field[0:3] = middle[held - 3 : held]
        field[3] = first[0]
        field[4:7] = ends[...]

    row_sums(field, sums, range(7), rows + TILE)
    base = side * (layers - 3)
    for row in range(0, rows, TILE):
        for layer in range(3):
            filtered = cone_tile(field, sums, layer + 2, row)
            for part, value in zip(parts_of(depth), filtered):
                alive = free_of(void[base + layer, row : row + TILE, part])
                result[layer, row : row + TILE, part] = alive * value


def near_kernel(void, first, middle, ends, result, field, sums):
    side_rows(lax.axis_index("lc"), void, first, middle, ends, result, field, sums)


def far_kernel(void, first, middle, ends, inner, near, gradient, field, sums, far, sems):
    layers = void.shape[0]
    core = lax.axis_index("lc")
    copies = [
        pltpu.make_async_copy(inner, gradient.at[pl.ds(3, layers - 6)], sems.at[0]),
        pltpu.make_async_copy(near, gradient.at[pl.ds(core * (layers - 3), 3)], sems.at[1]),
        pltpu.make_async_copy(far, gradient.at[pl.ds((1 - core) * (layers - 3), 3)], sems.at[2]),
    ]
    for copy in copies[:2]:
        copy.start()
    side_rows(1 - core, void, first, middle, ends, far, field, sums)
    copies[2].start()
    for copy in copies:
        copy.wait()


def vmem():
    return pl.BlockSpec(memory_space=pltpu.VMEM)


def hbm():
    return pl.BlockSpec(memory_space=pltpu.HBM)


def call(kernel, outs, scratch, in_specs, flops, out_specs=None, sems=0, limit=24 << 20):
    scratch = [pltpu.VMEM(shape, kind) for shape, kind in scratch]
    if sems:
        scratch.append(pltpu.SemaphoreType.DMA((sems,)))
    return pl.pallas_call(
        kernel,
        out_shape=[jax.ShapeDtypeStruct(shape, jnp.float32) for shape in outs],
        in_specs=in_specs,
        out_specs=out_specs or [vmem()] * len(outs),
        scratch_shapes=scratch,
        cost_estimate=pl.CostEstimate(flops=flops, bytes_accessed=1 << 20, transcendentals=0),
        compiler_params=pltpu.CompilerParams(vmem_limit_bytes=limit),
    )


def shards(density, void_mask, fixed_mask, displacement, load_ratio):
    layers, rows, depth = density.shape
    wide = rows + TILE
    gz, gy, lc = (lax.axis_size(axis) for axis in ("gz", "gy", "lc"))
    real = jnp.float32
    load_ratio = load_ratio.reshape(-1, 1)
    swap = [(0, 1), (1, 0)]
    across = []
    for z in range(1, gz):
        across.append((z * lc, (z - 1) * lc + 1))
        across.append(((z - 1) * lc + 1, z * lc))

    def y_pairs(step):
        if gy == 2:
            return [(y, 1 - y) for y in range(gy)]
        return [(y, y + step) for y in range(gy) if 0 <= y + step < gy]

    parts = lax.axis_size("parts")
    axes = ("parts", "gz", "gy", "lc")

    def at(part, place, y):
        return ((part * gz + place // lc) * gy + y) * lc + place % lc

    swaps = []
    if parts % 2 == 0:
        for part in range(parts):
            for place in (0, gz * lc - 1):
                swaps += [(at(part, place, y), at(part ^ 1, place, y)) for y in range(gy)]

    def across_pairs(peers):
        return [
            (at(part, a, y), at(part, b, peer)) for part in range(parts) for a, b in across for y, peer in peers
        ]

    crossing = across_pairs([(y, y) for y in range(gy)]) + swaps

    def diagonal(step):
        pairs = across_pairs(y_pairs(step))
        return pairs + swaps if gy == 2 else pairs

    sides, steps = (["both"], [1]) if gy == 2 else (["first", "last"], [-1, 1])
    count = len(sides)

    kinds = [
        ((3, rows, depth), real),
        ((rows, depth), jnp.int32),
        ((count, 3, layers, TILE, depth), real),
        ((count, layers, TILE, depth), jnp.int32),
        ((count, layers, TILE, depth), real),
        ((count, layers, TILE, depth), jnp.int32),
    ]
    crossing_out, *edges = call(
        functools.partial(prepare_kernel, sides),
        [(5, rows, depth)]
        + [(size, SLOT, depth) for size in (5, 3 * FIRST, 5 * layers - 3 * FIRST) for _ in sides],
        kinds,
        [hbm()] * 4,
        1 << 18,
        sems=3 + 4 * count,
        limit=PREPARE_LIMIT,
    )(displacement, fixed_mask, density, void_mask)
    crossed = lax.ppermute(crossing_out, axes, crossing)
    corners = [lax.ppermute(a, axes, diagonal(step)) for a, step in zip(edges[:count], steps)][::-1]
    halos, rests = (
        [lax.ppermute(a, "gy", y_pairs(step)) for a, step in zip(packs, steps)][::-1]
        for packs in (edges[count : 2 * count], edges[2 * count :])
    )

    def energy(kernel, held, high, low, outs, *more):
        return call(
            kernel,
            outs,
            [((3, held, high, depth), real), ((held, 6, high, depth), real)] + low,
            [vmem()] * (3 + len(more)),
            1 << 23,
        )(displacement, fixed_mask, load_ratio, *more)

    def scaling(kernel, held, *more):
        (made,) = call(
            functools.partial(kernel, count),
            [(held, wide, depth)],
            [((held + 4, wide, depth), real), ((held + 4, 2, wide, depth), real), ((held, TILE, depth), real)],
            [vmem()] * (2 + len(more)),
            1 << 21,
        )(density, void_mask, *more)
        return made

    (bulk,) = energy(energy_bulk_kernel, FIRST, rows, [], [(3, rows - TILE, depth)])
    mine, theirs = energy(
        functools.partial(energy_first_kernel, count),
        FIRST,
        3 * TILE,
        [((3, 2 * TILE, depth), real)],
        [(2, wide, depth), (5, wide, depth)],
        bulk,
        *halos,
    )
    received = lax.ppermute(theirs, "lc", swap)
    scaling_rest = scaling(scaling_rest_kernel, layers - 4, *rests)
    (mine_rest,) = energy(
        functools.partial(energy_rest_kernel, count),
        layers - 3,
        wide,
        [],
        [(layers - 4, wide, depth)],
        *halos,
        *rests,
    )
    (crown,) = energy(
        functools.partial(crown_kernel, count), 1, wide, [], [(1, wide, depth)], *halos
    )
    received_rest = lax.ppermute(mine_rest, "lc", swap)
    scaling_first = scaling(scaling_first_kernel, 2, crossed, *rests, *corners)
    first, outgoing = call(
        functools.partial(sensed_first_kernel, count),
        [(2, wide, depth), (3, wide, depth)],
        [((3, 2, wide, depth), real), ((2, 6, wide, depth), real)],
        [vmem()] * (5 + count),
        1 << 22,
    )(scaling_first, mine, received, load_ratio, crossed, *corners)
    (middle,) = call(
        sensed_rest_kernel, [(layers - 4, wide, depth)], [], [vmem()] * 3, 1 << 18
    )(scaling_rest, mine_rest, received_rest)
    beyond = lax.ppermute(outgoing, axes, crossing)
    other = lax.ppermute(first, "lc", swap)
    (inner,) = call(
        inner_kernel,
        [(layers - 6, rows, depth)],
        [((layers, wide, depth), real), ((layers, 2, wide, depth), real)],
        [vmem()] * 4,
        1 << 22,
    )(void_mask, first, other, middle)
    (own_ends,) = call(ends_kernel, [(3, wide, depth)], [], [vmem()] * 4, 1 << 18)(
        scaling_first, crown, outgoing, beyond
    )
    other_ends = lax.ppermute(own_ends, "lc", swap)
    held = [((7, wide, depth), real), ((7, 2, wide, depth), real)]
    (near,) = call(near_kernel, [(3, rows, depth)], held, [vmem()] * 4, 1 << 21)(
        void_mask, first, middle, own_ends
    )
    (gradient,) = call(
        far_kernel,
        [(layers, rows, depth)],
        held + [((3, rows, depth), real)],
        [vmem()] * 6,
        1 << 21,
        out_specs=[hbm()],
        sems=3,
    )(void_mask, other, middle, other_ends, inner, near)
    return gradient


def solution(mesh):
    placed = (
        P(("parts", "gz"), "gy", None),
        P(("parts", "gz"), "gy", None),
        P(("parts", "gz"), "gy", None),
        P("lc", None, ("parts", "gz"), "gy", None),
        P("parts"),
    )
    return jax.shard_map(
        shards,
        mesh=mesh,
        in_specs=placed,
        out_specs=P(("parts", "gz"), "gy", None),
        check_vma=False,
    )
```

```python
import functools
import math

import jax
import jax.numpy as jnp
from jax import lax
from jax.experimental import pallas as pl
from jax.experimental.pallas import tpu as pltpu
from jax.sharding import PartitionSpec as P

TILE = 8
SLOT = 4
LANES = 128
PREPARE_LIMIT = 53 << 20
WEIGHT = [2.5 - math.sqrt(squared) for squared in range(7)]


def energy_factors():
    poisson = 0.3
    factor = 1.0 / ((1.0 + poisson) * (1.0 - 2.0 * poisson))
    shear = factor * (0.5 - poisson) / 16.0
    bulk = factor * poisson / 16.0
    twist = factor * (0.5 - poisson) / 48.0
    warp = factor * ((1.0 - poisson) + 2.0 * (0.5 - poisson)) / 144.0
    return shear, bulk, twist, warp


def filled(shape, value=0.0):
    return jnp.full(shape, value, jnp.float32)


def lane_index():
    return lax.broadcasted_iota(jnp.int32, (TILE, LANES), 1)


def row_index():
    return lax.broadcasted_iota(jnp.int32, (TILE, LANES), 0)


def parts_of(depth):
    return [slice(at, at + LANES) for at in range(0, depth, LANES)]


def along_depth(values, offset):
    lane = lane_index()
    turned = [pltpu.roll(value, (-offset) % LANES, 1) for value in values]
    zero = filled((TILE, LANES))
    if offset > 0:
        keep, beyond = lane < LANES - offset, turned[1:] + [zero]
    else:
        keep, beyond = lane >= -offset, [zero] + turned[:-1]
    return [jnp.where(keep, own, other) for own, other in zip(turned, beyond)]


def along_rows(tiles, offset):
    turned = [pltpu.roll(tile, (-offset) % TILE, 0) for tile in tiles]
    if offset > 0:
        keep, beyond = row_index() < TILE - offset, turned[1:] + turned[:1]
    else:
        keep, beyond = row_index() >= -offset, turned[-1:] + turned[:-1]
    return [jnp.where(keep, own, other) for own, other in zip(turned, beyond)]


def row_sums(source, sums, layers, wide):
    depth = source.shape[-1]
    for layer in layers:
        for part in parts_of(depth):
            tiles = [source[layer, row : row + TILE, part] for row in range(0, wide, TILE)]
            for number, distance in enumerate((1, 2)):
                ahead, behind = along_rows(tiles, distance), along_rows(tiles, -distance)
                for index, (one, other) in enumerate(zip(ahead, behind)):
                    sums[layer, number, TILE * index : TILE * (index + 1), part] = one + other


def depth_levels(plain, near, corner, far, knight):
    w = WEIGHT
    level0 = w[0] * plain + w[1] * near + w[2] * corner + w[4] * far + w[5] * knight
    level1 = w[1] * plain + w[2] * near + w[3] * corner + w[5] * far + w[6] * knight
    level2 = w[4] * plain + w[5] * near + w[6] * corner
    return level0, level1, level2


def cone_tile(source, sums, layer, row):
    results = []
    for part in parts_of(source.shape[-1]):

        def plane(at):
            return source[layer + at, row : row + TILE, part]

        def summed(at, number):
            return sums[layer + at, number, row : row + TILE, part]

        near = (plane(-1) + plane(1)) + summed(0, 0)
        corner = summed(-1, 0) + summed(1, 0)
        far = (plane(-2) + plane(2)) + summed(0, 1)
        knight = (summed(-1, 1) + summed(1, 1)) + (summed(-2, 0) + summed(2, 0))
        results.append(depth_levels(plane(0), near, corner, far, knight))
    level1 = [levels[1] for levels in results]
    level2 = [levels[2] for levels in results]
    shifted = [along_depth(level1, 1), along_depth(level1, -1), along_depth(level2, 2), along_depth(level2, -2)]
    return [
        levels[0] + ((one + two) + (three + four))
        for levels, one, two, three, four in zip(results, *shifted)
    ]


def row_modes(nodes, modes, layer, slot, wide):
    for component in range(3):
        for part in parts_of(nodes.shape[-1]):
            tiles = [nodes[component, layer, row : row + TILE, part] for row in range(0, wide, TILE)]
            for index, (low, high) in enumerate(zip(tiles, along_rows(tiles, 1))):
                at = slice(TILE * index, TILE * (index + 1))
                modes[slot, 2 * component, at, part] = low + high
                modes[slot, 2 * component + 1, at, part] = high - low


def node_modes(modes, slot, row):
    parts = parts_of(modes.shape[-1])
    found = [[] for _ in parts]
    for number in range(6):
        values = [modes[slot, number, row : row + TILE, part] for part in parts]
        for mine, value, after in zip(found, values, along_depth(values, 1)):
            mine.append(value + after)
            mine.append(after - value)
    return found


def element_energy(lower, upper, scale):
    def mode(component, first, second, third):
        index = 4 * component + 2 * second + third
        if first:
            return upper[index] - lower[index]
        return upper[index] + lower[index]

    def square(value):
        return value * value

    normal = [mode(0, 1, 0, 0), mode(1, 0, 1, 0), mode(2, 0, 0, 1)]
    trace = normal[0] + normal[1] + normal[2]
    main = square(mode(0, 0, 0, 1) + mode(2, 1, 0, 0))
    main = main + square(mode(1, 0, 0, 1) + mode(2, 0, 1, 0))
    main = main + square(mode(0, 0, 1, 0) + mode(1, 1, 0, 0))
    bent = [
        (mode(1, 0, 1, 1), mode(0, 1, 0, 1)),
        (mode(2, 0, 1, 1), mode(0, 1, 1, 0)),
        (mode(2, 1, 0, 1), mode(1, 1, 1, 0)),
    ]
    half = None
    for left, right in bent:
        main = main + square(left + right)
        term = square(left - right)
        half = term if half is None else half + term
    main = main + 2.0 * (square(normal[0]) + square(normal[1]) + square(normal[2]))
    main = main + 0.5 * half
    twisted = [mode(0, 0, 1, 1), mode(1, 1, 0, 1), mode(2, 1, 1, 0)]
    twists = square(twisted[0]) + square(twisted[1]) + square(twisted[2])
    twists = twists + square(twisted[0] + twisted[1] + twisted[2])
    warps = square(mode(0, 1, 1, 1)) + square(mode(1, 1, 1, 1)) + square(mode(2, 1, 1, 1))
    shear, bulk, twist, warp = scale
    return (shear * main + bulk * square(trace)) + (twist * twists + warp * warps)


def shares(ratio):
    values = [jnp.broadcast_to(ratio[case : case + 1, :], (TILE, LANES)) for case in range(ratio.shape[0])]
    values = [value.astype(jnp.float32) for value in values]
    total = values[0]
    for value in values[1:]:
        total = total + value

    def scale(case):
        chosen = values[0]
        for number, value in enumerate(values[1:], 1):
            chosen = jnp.where(case == number, value, chosen)
        share = chosen / total
        return [factor * share for factor in energy_factors()]

    return scale


def flag(condition):
    return jnp.where(condition, 1.0, 0.0).astype(jnp.float32)


def y_flags():
    rank = lax.axis_index("gy")
    return flag(rank > 0), flag(rank < lax.axis_size("gy") - 1)


def beyond_flag():
    rank, core = lax.axis_index("gz"), lax.axis_index("lc")
    return flag((rank > 0) & (core == 0) | (rank < lax.axis_size("gz") - 1) & (core == 1))


def free_of(mask):
    return (1 - mask).astype(jnp.float32)


def edge_of(first, last, side):
    if side == "both":
        return jnp.where(lax.axis_index("gy") == 0, pltpu.roll(last, SLOT, 0), first)[0:SLOT]
    return first[0:SLOT] if side == "first" else pltpu.roll(last, SLOT, 0)[0:SLOT]


def prepare_kernel(sides, displacement, fixed, density, void, *refs):
    count = len(sides)
    crossing, corners, firsts, rests = (refs[0], *(refs[1 + at * count : 1 + (at + 1) * count] for at in range(3)))
    nodes, mask, node_edge, mask_edge, design_edge, void_edge, sems = refs[1 + 3 * count :]
    layers, rows, _ = density.shape
    core = lax.axis_index("lc")
    layer_out = core * (layers - 1)
    copies = [
        pltpu.make_async_copy(displacement.at[0, :, layer_out], nodes, sems.at[0]),
        pltpu.make_async_copy(fixed.at[layer_out], mask, sems.at[1]),
        pltpu.make_async_copy(
            density.at[pl.ds(core * (layers - 2), 2)], crossing.at[pl.ds(3, 2)], sems.at[2]
        ),
    ]
    for number, side in enumerate(sides):
        if side == "both":
            start = pl.multiple_of((1 - lax.axis_index("gy")) * (rows - TILE), TILE)
        else:
            start = 0 if side == "first" else rows - TILE
        at = pl.ds(start, TILE)
        base = 3 + 4 * number
        copies += [
            pltpu.make_async_copy(displacement.at[0, :, :, at], node_edge.at[number], sems.at[base]),
            pltpu.make_async_copy(fixed.at[:, at], mask_edge.at[number], sems.at[base + 1]),
            pltpu.make_async_copy(density.at[:, at], design_edge.at[number], sems.at[base + 2]),
            pltpu.make_async_copy(void.at[:, at], void_edge.at[number], sems.at[base + 3]),
        ]
    for copy in copies:
        copy.start()
    for copy in copies:
        copy.wait()
    free = free_of(mask[...])
    for component in range(3):
        crossing[component] = nodes[component] * free
    for side, corner in zip(sides, corners):
        for index in range(5):
            corner[index] = edge_of(crossing[index, 0:TILE, :], crossing[index, rows - TILE : rows, :], side)
    early = first_layers(layers)
    for number, (side, first, rest) in enumerate(zip(sides, firsts, rests)):
        base = 3 * (layers - FIRST)
        for layer in range(layers):
            free = free_of(mask_edge[number, layer])
            for component in range(3):
                moved = free * node_edge[number, component, layer]
                if layer in early:
                    first[component * FIRST + early.index(layer)] = edge_of(moved, moved, side)
                else:
                    rest[component * (layers - FIRST) + layer - 3] = edge_of(moved, moved, side)
            design = design_edge[number, layer]
            rest[base + layer] = edge_of(design, design, side)
            alive = free_of(void_edge[number, layer])
            rest[base + layers + layer] = edge_of(alive, alive, side)


FIRST = 5


def first_layers(layers):
    return (0, 1, 2, layers - 2, layers - 1)


def node_halo(firsts, rests, component, layer, layers):
    early = first_layers(layers)
    if layer in early:
        at, packs = component * FIRST + early.index(layer), firsts
    else:
        at, packs = component * (layers - FIRST) + layer - 3, rests
    return packs[0][at], packs[-1][at]


def load_nodes(displacement, fixed, firsts, rests, layer, nodes, modes, slot):
    layers, rows, _ = fixed.shape
    wide = rows + TILE
    has_left, has_right = y_flags()
    free = free_of(fixed[layer])
    for component in range(3):
        nodes[component, slot, 0:rows, :] = displacement[0, component, layer] * free
        left, right = node_halo(firsts, rests, component, layer, layers)
        nodes[component, slot, rows : rows + SLOT, :] = right * has_right
        nodes[component, slot, rows + SLOT : wide, :] = left * has_left
    row_modes(nodes, modes, slot, slot, wide)


def first_energy(modes, energy, tiles, scale):
    depth = energy.shape[-1]
    for row in range(0, TILE * tiles, TILE):
        found = [node_modes(modes, slot, row) for slot in range(FIRST)]
        for index, slot in enumerate((0, 1, 3)):
            for part, below, above in zip(parts_of(depth), found[slot], found[slot + 1]):
                energy[index, row : row + TILE, part] = element_energy(below, above, scale)


def energy_bulk_kernel(displacement, fixed, ratio, energy, nodes, modes):
    layers, rows, _ = fixed.shape
    for slot, layer in enumerate(first_layers(layers)):
        free = free_of(fixed[layer])
        for component in range(3):
            nodes[component, slot] = displacement[0, component, layer] * free
        row_modes(nodes, modes, slot, slot, rows)
    scale = shares(ratio)(lax.axis_index("lc"))
    first_energy(modes, energy, rows // TILE - 1, scale)


def energy_first_kernel(count, displacement, fixed, ratio, bulk, *refs):
    halos = refs[:count]
    mine, theirs, nodes, modes, energy = refs[count:]
    layers, rows, _ = fixed.shape
    last = rows - TILE
    core = lax.axis_index("lc")
    has_left, has_right = y_flags()
    for slot, layer in enumerate(first_layers(layers)):
        free = free_of(fixed[layer, last:rows])
        free_next = free_of(fixed[layer, 0:TILE])
        for component in range(3):
            left, right = node_halo(halos, None, component, layer, layers)
            nodes[component, slot, 0:TILE, :] = displacement[0, component, layer, last:rows] * free
            nodes[component, slot, TILE : TILE + SLOT, :] = right * has_right
            nodes[component, slot, TILE + SLOT : 2 * TILE, :] = left * has_left
            nodes[component, slot, 2 * TILE : 3 * TILE, :] = displacement[0, component, layer, 0:TILE] * free_next
        row_modes(nodes, modes, slot, slot, 3 * TILE)
    first_energy(modes, energy, 2, shares(ratio)(core))

    def whole_layer(target, index, source):
        target[index, 0:last, :] = bulk[source]
        target[index, last : rows + TILE, :] = energy[source]

    def node_layer(layer, slot):
        free = free_of(fixed[layer])
        for component in range(3):
            theirs[2 + component, 0:rows, :] = displacement[0, component, layer] * free
            theirs[2 + component, rows : rows + TILE, :] = nodes[component, slot, TILE : 2 * TILE, :]

    @pl.when(core == 0)
    def _():
        whole_layer(mine, 0, 0)
        whole_layer(mine, 1, 1)
        whole_layer(theirs, 0, 2)
        whole_layer(theirs, 1, 2)
        node_layer(layers - 1, FIRST - 1)

    @pl.when(core == 1)
    def _():
        whole_layer(mine, 0, 2)
        whole_layer(mine, 1, 2)
        whole_layer(theirs, 0, 0)
        whole_layer(theirs, 1, 1)
        node_layer(0, 0)


def energy_rest_kernel(count, displacement, fixed, ratio, *refs):
    firsts, rests = refs[:count], refs[count : 2 * count]
    energy, nodes, modes = refs[2 * count :]
    layers, rows, depth = fixed.shape
    wide = rows + TILE
    core = lax.axis_index("lc")
    for slot in range(layers - 3):
        load_nodes(displacement, fixed, firsts, rests, slot + 2, nodes, modes, slot)
    scale = shares(ratio)(core)
    for row in range(0, wide, TILE):
        lower = node_modes(modes, 0, row)
        for layer in range(layers - 4):
            upper = node_modes(modes, layer + 1, row)
            for part, below, above in zip(parts_of(depth), lower, upper):
                energy[layer, row : row + TILE, part] = element_energy(below, above, scale)
            lower = upper


def crown_kernel(count, displacement, fixed, ratio, *refs):
    firsts = refs[:count]
    crown, nodes, modes = refs[count:]
    layers, rows, depth = fixed.shape
    wide = rows + TILE
    core = lax.axis_index("lc")
    crown[0] = filled((wide, depth))

    @pl.when((core == 1) & (lax.axis_index("gz") == lax.axis_size("gz") - 1))
    def _():
        scale = shares(ratio)(core)
        load_nodes(displacement, fixed, firsts, None, layers - 1, nodes, modes, 0)
        zero = [filled((TILE, LANES))] * 12
        for row in range(0, wide, TILE):
            for part, below in zip(parts_of(depth), node_modes(modes, 0, row)):
                crown[0, row : row + TILE, part] = element_energy(below, zero, scale)


def place(design, slot, middle, left, right, keep=1.0):
    rows = middle.shape[0]
    has_left, has_right = y_flags()
    design[slot, 0:rows, :] = middle * keep
    design[slot, rows : rows + SLOT, :] = right * (keep * has_right)
    design[slot, rows + SLOT : rows + TILE, :] = left * (keep * has_left)


def scaling_first_kernel(count, density, void, beyond, *refs):
    halos, corners = refs[:count], refs[count : 2 * count]
    scaling, design, sums, halo_alive = refs[2 * count :]
    layers = density.shape[0]
    core = lax.axis_index("lc")
    has_beyond = beyond_flag()
    for index in range(4):
        source = index + core * (layers - 4)
        at = 3 * (layers - FIRST) + source
        place(design, index + 2 * (1 - core), density[source], halos[0][at], halos[-1][at])
    for index in range(2):
        at = 3 + index
        place(design, 4 * core + index, beyond[at], corners[0][at], corners[-1][at], has_beyond)
    scale_layers(core * (layers - 2), void, halos, scaling, design, sums, halo_alive)


def scaling_rest_kernel(count, density, void, *refs):
    halos = refs[:count]
    scaling, design, sums, halo_alive = refs[count:]
    layers = density.shape[0]
    for layer in range(layers):
        at = 3 * (layers - FIRST) + layer
        place(design, layer, density[layer], halos[0][at], halos[-1][at])
    scale_layers(2, void, halos, scaling, design, sums, halo_alive)


def scale_layers(start, void, halos, scaling, design, sums, halo_alive):
    layers, rows, depth = void.shape
    half = scaling.shape[0]
    wide = rows + TILE
    has_left, has_right = y_flags()
    for layer in range(half):
        at = 3 * (layers - FIRST) + layers + start + layer
        halo_alive[layer, 0:SLOT, :] = halos[-1][at] * has_right
        halo_alive[layer, SLOT:TILE, :] = halos[0][at] * has_left
    row_sums(design, sums, range(half + 4), wide)

    total_x = layers * lax.axis_size("gz")
    total_y = rows * lax.axis_size("gy")
    first_layer = lax.axis_index("gz") * layers + start
    first_row = lax.axis_index("gy") * rows
    parts = parts_of(depth)
    lane = lane_index()

    def depth_count(number, distance):
        held = filled((TILE, LANES), 2.0)
        if number == 0:
            held = jnp.where(lane < distance, 1.0, held)
        if number == len(parts) - 1:
            held = jnp.where(lane >= LANES - distance, held - 1.0, held)
        return held

    counts = [(depth_count(number, 1), depth_count(number, 2)) for number in range(len(parts))]

    def inside(at):
        return flag((at >= 0) & (at < total_x))

    for row in range(0, wide, TILE):
        column = row_index() + (first_row + row)
        if row == rows:
            column = jnp.where(row_index() >= SLOT, column - (rows + TILE), column)

        def within(offset):
            at = column + offset
            return jnp.where((at >= 0) & (at < total_y), 1.0, 0.0)

        y0, y1, y2 = within(0), within(-1) + within(1), within(-2) + within(2)
        for layer in range(half):
            filtered = cone_tile(design, sums, layer + 2, row)
            at = first_layer + layer
            x1 = inside(at - 1) + inside(at + 1)
            x2 = inside(at - 2) + inside(at + 2)
            level0, level1, level2 = depth_levels(
                y0, x1 * y0 + y1, x1 * y1, x2 * y0 + y2, x1 * y2 + x2 * y1
            )
            for part, value, (count1, count2) in zip(parts, filtered, counts):
                weight_sum = jnp.maximum(level0 + count1 * level1 + count2 * level2, 1.0)
                inverse = 1.0 / weight_sum
                physical = value * inverse
                value = (-3.0 * (1.0 - 0.001)) * physical * physical * inverse
                if row == rows:
                    alive = halo_alive[layer, :, part]
                else:
                    alive = free_of(void[start + layer, row : row + TILE, part])
                scaling[layer, row : row + TILE, part] = value * alive


def sensed_first_kernel(count, scaling, mine, received, ratio, crossed, *refs):
    corners = refs[:count]
    sensed, outgoing, nodes, modes = refs[count:]
    _, wide, depth = scaling.shape
    rows = wide - TILE
    core = lax.axis_index("lc")
    has_left, has_right = y_flags()
    has_beyond = beyond_flag()
    for component in range(3):
        nodes[component, core, 0:rows, :] = crossed[component] * has_beyond
        nodes[component, core, rows : rows + SLOT, :] = corners[-1][component] * (has_beyond * has_right)
        nodes[component, core, rows + SLOT : wide, :] = corners[0][component] * (has_beyond * has_left)
        nodes[component, 1 - core] = received[2 + component]
    for index in range(2):
        row_modes(nodes, modes, index, index, wide)
    scale = shares(ratio)(1 - core)
    between = 2 - core
    for row in range(0, wide, TILE):
        lower, upper = (node_modes(modes, index, row) for index in (0, 1))
        for part, below, above in zip(parts_of(depth), lower, upper):
            outgoing[between, row : row + TILE, part] = element_energy(below, above, scale)
    for layer in range(2):
        sensed[layer] = scaling[layer] * (mine[layer] + received[layer])

    @pl.when(core == 0)
    def _():
        outgoing[0:2] = sensed[0:2]

    @pl.when(core == 1)
    def _():
        outgoing[0] = sensed[0]
        outgoing[2] = scaling[1]


def sensed_rest_kernel(scaling, mine, received, sensed):
    for layer in range(scaling.shape[0]):
        sensed[layer] = scaling[layer] * (mine[layer] + received[layer])


def ends_kernel(scaling, crown, outgoing, received, ends):
    core = lax.axis_index("lc")

    has_beyond = beyond_flag()

    @pl.when(core == 0)
    def _():
        ends[0] = has_beyond * received[0]
        ends[1] = has_beyond * (received[2] * (received[1] + outgoing[2]))
        ends[2] = received[0]

    @pl.when(core == 1)
    def _():
        ends[0] = scaling[1] * ((outgoing[1] + crown[0]) + has_beyond * received[2])
        ends[1] = has_beyond * received[0]
        ends[2] = has_beyond * received[1]


def inner_kernel(void, own, other, middle, gradient, field, sums):
    layers, rows, depth = void.shape
    core = lax.axis_index("lc")
    field[pl.ds(core * (layers - 2), 2)] = own[...]
    field[pl.ds((1 - core) * (layers - 2), 2)] = other[...]
    field[2 : layers - 2] = middle[...]
    row_sums(field, sums, range(1, layers - 1), rows + TILE)
    for row in range(0, rows, TILE):
        for layer in range(3, layers - 3):
            filtered = cone_tile(field, sums, layer, row)
            for part, value in zip(parts_of(depth), filtered):
                alive = free_of(void[layer, row : row + TILE, part])
                gradient[layer - 3, row : row + TILE, part] = alive * value


def side_rows(side, void, first, middle, ends, result, field, sums):
    layers, rows, depth = void.shape
    held = middle.shape[0]

    @pl.when(side == 0)
    def _():
        field[0:2] = ends[0:2]
        field[2:4] = first[...]
        field[4:7] = middle[0:3]

    @pl.when(side == 1)
    def _():
        field[0:3] = middle[held - 3 : held]
        field[3] = first[0]
        field[4:7] = ends[...]

    row_sums(field, sums, range(7), rows + TILE)
    base = side * (layers - 3)
    for row in range(0, rows, TILE):
        for layer in range(3):
            filtered = cone_tile(field, sums, layer + 2, row)
            for part, value in zip(parts_of(depth), filtered):
                alive = free_of(void[base + layer, row : row + TILE, part])
                result[layer, row : row + TILE, part] = alive * value


def near_kernel(void, first, middle, ends, result, field, sums):
    side_rows(lax.axis_index("lc"), void, first, middle, ends, result, field, sums)


def gather_kernel(inner, near, far, gradient, sems):
    layers = gradient.shape[0]
    core = lax.axis_index("lc")
    copies = [
        pltpu.make_async_copy(inner, gradient.at[pl.ds(3, layers - 6)], sems.at[0]),
        pltpu.make_async_copy(near, gradient.at[pl.ds(core * (layers - 3), 3)], sems.at[1]),
        pltpu.make_async_copy(far, gradient.at[pl.ds((1 - core) * (layers - 3), 3)], sems.at[2]),
    ]
    for copy in copies:
        copy.start()
    for copy in copies:
        copy.wait()


def vmem():
    return pl.BlockSpec(memory_space=pltpu.VMEM)


def hbm():
    return pl.BlockSpec(memory_space=pltpu.HBM)


def call(kernel, outs, scratch, in_specs, flops, out_specs=None, sems=0, limit=24 << 20):
    scratch = [pltpu.VMEM(shape, kind) for shape, kind in scratch]
    if sems:
        scratch.append(pltpu.SemaphoreType.DMA((sems,)))
    return pl.pallas_call(
        kernel,
        out_shape=[jax.ShapeDtypeStruct(shape, jnp.float32) for shape in outs],
        in_specs=in_specs,
        out_specs=out_specs or [vmem()] * len(outs),
        scratch_shapes=scratch,
        cost_estimate=pl.CostEstimate(flops=flops, bytes_accessed=1 << 20, transcendentals=0),
        compiler_params=pltpu.CompilerParams(vmem_limit_bytes=limit),
    )


def shards(density, void_mask, fixed_mask, displacement, load_ratio):
    layers, rows, depth = density.shape
    wide = rows + TILE
    gz, gy, lc = (lax.axis_size(axis) for axis in ("gz", "gy", "lc"))
    real = jnp.float32
    load_ratio = load_ratio.reshape(-1, 1)
    swap = [(0, 1), (1, 0)]
    across = []
    for z in range(1, gz):
        across.append((z * lc, (z - 1) * lc + 1))
        across.append(((z - 1) * lc + 1, z * lc))

    def y_pairs(step):
        if gy == 2:
            return [(y, 1 - y) for y in range(gy)]
        return [(y, y + step) for y in range(gy) if 0 <= y + step < gy]

    parts = lax.axis_size("parts")
    axes = ("parts", "gz", "gy", "lc")

    def at(part, place, y):
        return ((part * gz + place // lc) * gy + y) * lc + place % lc

    swaps = []
    if parts % 2 == 0:
        for part in range(parts):
            for place in (0, gz * lc - 1):
                swaps += [(at(part, place, y), at(part ^ 1, place, y)) for y in range(gy)]

    def across_pairs(peers):
        return [
            (at(part, a, y), at(part, b, peer)) for part in range(parts) for a, b in across for y, peer in peers
        ]

    crossing = across_pairs([(y, y) for y in range(gy)]) + swaps

    def diagonal(step):
        pairs = across_pairs(y_pairs(step))
        return pairs + swaps if gy == 2 else pairs

    sides, steps = (["both"], [1]) if gy == 2 else (["first", "last"], [-1, 1])
    count = len(sides)

    kinds = [
        ((3, rows, depth), real),
        ((rows, depth), jnp.int32),
        ((count, 3, layers, TILE, depth), real),
        ((count, layers, TILE, depth), jnp.int32),
        ((count, layers, TILE, depth), real),
        ((count, layers, TILE, depth), jnp.int32),
    ]
    crossing_out, *edges = call(
        functools.partial(prepare_kernel, sides),
        [(5, rows, depth)]
        + [(size, SLOT, depth) for size in (5, 3 * FIRST, 5 * layers - 3 * FIRST) for _ in sides],
        kinds,
        [hbm()] * 4,
        1 << 18,
        sems=3 + 4 * count,
        limit=PREPARE_LIMIT,
    )(displacement, fixed_mask, density, void_mask)
    crossed = lax.ppermute(crossing_out, axes, crossing)
    corners = [lax.ppermute(a, axes, diagonal(step)) for a, step in zip(edges[:count], steps)][::-1]
    halos, rests = (
        [lax.ppermute(a, "gy", y_pairs(step)) for a, step in zip(packs, steps)][::-1]
        for packs in (edges[count : 2 * count], edges[2 * count :])
    )

    def energy(kernel, held, high, low, outs, *more):
        return call(
            kernel,
            outs,
            [((3, held, high, depth), real), ((held, 6, high, depth), real)] + low,
            [vmem()] * (3 + len(more)),
            1 << 23,
        )(displacement, fixed_mask, load_ratio, *more)

    def scaling(kernel, held, *more):
        (made,) = call(
            functools.partial(kernel, count),
            [(held, wide, depth)],
            [((held + 4, wide, depth), real), ((held + 4, 2, wide, depth), real), ((held, TILE, depth), real)],
            [vmem()] * (2 + len(more)),
            1 << 21,
        )(density, void_mask, *more)
        return made

    (bulk,) = energy(energy_bulk_kernel, FIRST, rows, [], [(3, rows - TILE, depth)])
    mine, theirs = energy(
        functools.partial(energy_first_kernel, count),
        FIRST,
        3 * TILE,
        [((3, 2 * TILE, depth), real)],
        [(2, wide, depth), (5, wide, depth)],
        bulk,
        *halos,
    )
    received = lax.ppermute(theirs, "lc", swap)
    scaling_rest = scaling(scaling_rest_kernel, layers - 4, *rests)
    (mine_rest,) = energy(
        functools.partial(energy_rest_kernel, count), layers - 3, wide, [], [(layers - 4, wide, depth)], *halos, *rests
    )
    (crown,) = energy(functools.partial(crown_kernel, count), 1, wide, [], [(1, wide, depth)], *halos)
    received_rest = lax.ppermute(mine_rest, "lc", swap)
    scaling_first = scaling(scaling_first_kernel, 2, crossed, *rests, *corners)
    first, outgoing = call(
        functools.partial(sensed_first_kernel, count),
        [(2, wide, depth), (3, wide, depth)],
        [((3, 2, wide, depth), real), ((2, 6, wide, depth), real)],
        [vmem()] * (5 + count),
        1 << 22,
    )(scaling_first, mine, received, load_ratio, crossed, *corners)
    (middle,) = call(
        sensed_rest_kernel, [(layers - 4, wide, depth)], [], [vmem()] * 3, 1 << 18
    )(scaling_rest, mine_rest, received_rest)
    beyond = lax.ppermute(outgoing, axes, crossing)
    other = lax.ppermute(first, "lc", swap)
    (inner,) = call(
        inner_kernel,
        [(layers - 6, rows, depth)],
        [((layers, wide, depth), real), ((layers, 2, wide, depth), real)],
        [vmem()] * 4,
        1 << 22,
    )(void_mask, first, other, middle)
    (own_ends,) = call(ends_kernel, [(3, wide, depth)], [], [vmem()] * 4, 1 << 18)(
        scaling_first, crown, outgoing, beyond
    )
    held = [((7, wide, depth), real), ((7, 2, wide, depth), real)]
    (near,) = call(near_kernel, [(3, rows, depth)], held, [vmem()] * 4, 1 << 21)(void_mask, first, middle, own_ends)
    far = lax.ppermute(near, "lc", swap)
    (gradient,) = call(
        gather_kernel, [(layers, rows, depth)], [], [vmem()] * 3, 1 << 18, out_specs=[hbm()], sems=3
    )(inner, near, far)
    return gradient


def solution(mesh):
    placed = (
        P(("parts", "gz"), "gy", None),
        P(("parts", "gz"), "gy", None),
        P(("parts", "gz"), "gy", None),
        P("lc", None, ("parts", "gz"), "gy", None),
        P("parts"),
    )
    return jax.shard_map(
        shards,
        mesh=mesh,
        in_specs=placed,
        out_specs=P(("parts", "gz"), "gy", None),
        check_vma=False,
    )
```
